256 devices in a mesh: groups: 2 (over z), seq: 128 (over y, x, core).
Axes of the slice: x: 8, y: 8, z: 2, core: 2. Of those that a mesh axis runs over, the one named last changes fastest.
The devices are a block of a 8x8x16 slice.
Arguments:
- queries: bfloat16 [65536, 4096], P(('groups', 'seq')), parts along dimension 0, may hold values from -13 to 13
- keys: bfloat16 [65536, 512], P(('groups', 'seq')), parts along dimension 0, may hold values from -13 to 13
- values: bfloat16 [65536, 512], P(('groups', 'seq')), parts along dimension 0, may hold values from -6 to 6
- segment_ids: int32 [65536], P(('groups', 'seq')), parts along dimension 0, may hold values from 0 to 63, as said below
Outputs:
- attended: bfloat16 [65536, 4096], P(('groups', 'seq')), parts along dimension 0
- rotated_keys: bfloat16 [65536, 512], P(('groups', 'seq')), parts along dimension 0
The draws below stay inside these ranges and needn't reach their ends.
There are 2 independent parts, one for each index of `groups`. The reference program is written for one: setup_inputs(seed, part) draws one part's arguments, and reference() takes and returns one part's arrays. A program takes and returns all parts, laid end to end along the dimension named above; each array names one. Nothing has to cross between parts.
Inputs may be any that keep to these rules, and one draw needn't show every extreme that they name: `segment_ids`: never falling along the packed stream, starting at 0 and rising by one at each new rollout; each rollout covers 1 to 1792 tokens and one covers exactly 1792.
All inputs are finite; a program needn't handle non-finite values.
Results may differ from the reference program's by a relative error of at most 0.0054.
Values may be sent and summed in bfloat16 or wider, within the bound.
A program may use at most 192 MiB of HBM per device.

```python
import jax
import jax.numpy as jnp
from jax import lax

HQ = 32
HK = 4
HD = 128
SPAN = 7
TOK_DEV = 256
TOKENS = 32768
N_SEQ = 128


def base_draw(own_key, width):
    return jnp.clip(jax.random.normal(own_key, (TOKENS, width), jnp.float32), -6.0, 6.0)


def draw_queries(key, part):
    drawn = base_draw(jax.random.fold_in(key, 21), HQ * HD)
    return drawn.astype(jnp.bfloat16)


def draw_keys(key, part):
    drawn = base_draw(jax.random.fold_in(key, 22), HK * HD)
    return drawn.astype(jnp.bfloat16)


def draw_segment_ids(key, part):
    quarter = TOK_DEV // 4
    offset_key = jax.random.fold_in(key, 31)
    lead_offset = jax.random.randint(jax.random.fold_in(offset_key, 1), (), 1, quarter)
    first_cut = (N_SEQ // 2 - 1) * TOK_DEV + jax.random.randint(jax.random.fold_in(offset_key, 2), (), 1, TOK_DEV)
    second_cut = N_SEQ // 2 * TOK_DEV + jax.random.randint(jax.random.fold_in(offset_key, 3), (), 1, TOK_DEV)
    third_cut = (N_SEQ // 2 + 1) * TOK_DEV + jax.random.randint(jax.random.fold_in(offset_key, 4), (), 1, TOK_DEV)
    window_count = N_SEQ // 2
    window_number = jnp.arange(window_count, dtype=jnp.int32)
    window_shift = jax.random.randint(jax.random.fold_in(offset_key, 5), (window_count,), 0, TOK_DEV)
    window_place = window_number * (2 * TOK_DEV) + window_shift
    window_used = (window_number >= 4) & (window_number != N_SEQ // 4 - 1) & (window_number != N_SEQ // 4)
    window_place = jnp.where(window_used, window_place, 0)
    marks = jnp.zeros((TOKENS,), jnp.int32)
    marks = marks.at[window_place].max(window_used.astype(jnp.int32))
    marks = marks.at[0].set(1)
    marks = marks.at[lead_offset].set(1)
    marks = marks.at[lead_offset + SPAN * TOK_DEV].set(1)
    marks = marks.at[first_cut].set(1)
    marks = marks.at[second_cut].set(1)
    marks = marks.at[third_cut].set(1)
    return (jnp.cumsum(marks) - 1).astype(jnp.int32)


def shard_levels(key, shape, shards, smallest, top_value):
    def one(axis_at, blocks):
        heights = jax.random.uniform(jax.random.fold_in(jax.random.fold_in(key, 6), axis_at), (blocks,), jnp.float32, smallest / len(shards), top_value / len(shards))
        return jnp.repeat(jnp.exp(heights), shape[axis_at] // blocks).reshape((-1,) + (1,) * (len(shape) - axis_at - 1))

    loudness = one(*shards[0])
    for cut in shards[1:]:
        loudness = loudness * one(*cut)
    return loudness


def gaussian(rng, shape, deviation, most, split=(), kind=jnp.bfloat16):
    entries = deviation * jax.random.normal(rng, shape, jnp.float32)
    if split:
        entries = entries * shard_levels(rng, shape, split, -0.22, 0.18)
    return jnp.clip(entries, -most, most).astype(kind)


def setup_inputs(seed: int = 0, part: int = 0) -> dict:
    splits = jax.random.split(jax.random.key(seed), 5)
    part_splits = jax.random.split(jax.random.fold_in(splits[4], part), 5)
    queries = draw_queries(jax.random.fold_in(jax.random.fold_in(splits[4], part), 71), part)
    keys = draw_keys(jax.random.fold_in(jax.random.fold_in(splits[4], part), 71), part)
    values = gaussian(part_splits[2], (TOKENS, HK * HD), 1.0, 6.0, ((0, 128),))
    segment_ids = draw_segment_ids(jax.random.fold_in(jax.random.fold_in(splits[4], part), 71), part)
    return dict(queries=queries, keys=keys, values=values, segment_ids=segment_ids)


ROPE_BASE = 1000000.0
MASKED_SCORE = -1.0e30


def rollout_starts(segment_ids):
    token_index = jnp.arange(segment_ids.shape[0], dtype=jnp.int32)
    boundary = jnp.concatenate([jnp.ones((1,), dtype=jnp.bool_), segment_ids[1:] != segment_ids[:-1]])
    return lax.cummax(jnp.where(boundary, token_index, -1), axis=0)


def rotate_heads(matrix, positions, head_count):
    row_count = matrix.shape[0]
    half_dim = HD // 2
    inverse_freq = ROPE_BASE ** (-(jnp.arange(half_dim, dtype=jnp.float32) * (2.0 / HD)))
    angles = positions.astype(jnp.float32)[:, None] * inverse_freq[None, :]
    cosine = jnp.cos(angles)[:, None, :]
    sine = jnp.sin(angles)[:, None, :]
    split_heads = matrix.astype(jnp.float32).reshape(row_count, head_count, HD)
    lower_half = split_heads[..., :half_dim]
    upper_half = split_heads[..., half_dim:]
    turned = jnp.concatenate([lower_half * cosine - upper_half * sine, upper_half * cosine + lower_half * sine], axis=-1)
    return turned.reshape(row_count, head_count * HD).astype(jnp.bfloat16)


def reference(queries, keys, values, segment_ids):
    token_count = queries.shape[0]
    starts = rollout_starts(segment_ids)
    positions = jnp.arange(token_count, dtype=jnp.int32) - starts
    turned_queries = rotate_heads(queries, positions, HQ)
    rotated_keys = rotate_heads(keys, positions, HK)
    reach_rows = SPAN * TOK_DEV
    window_rows = (SPAN + 1) * TOK_DEV
    group_size = HQ // HK
    padded_keys = jnp.concatenate([jnp.zeros((reach_rows, HK * HD), jnp.bfloat16), rotated_keys], axis=0)
    padded_values = jnp.concatenate([jnp.zeros((reach_rows, HK * HD), jnp.bfloat16), values], axis=0)

    def one_block(block_number):
        block_first = (block_number * TOK_DEV).astype(jnp.int32)
        query_block = lax.dynamic_slice_in_dim(turned_queries, block_first, TOK_DEV, 0).astype(jnp.float32).reshape(TOK_DEV, HK, group_size, HD)
        key_window = lax.dynamic_slice_in_dim(padded_keys, block_first, window_rows, 0).astype(jnp.float32).reshape(window_rows, HK, HD)
        value_window = lax.dynamic_slice_in_dim(padded_values, block_first, window_rows, 0).astype(jnp.float32).reshape(window_rows, HK, HD)
        query_starts = lax.dynamic_slice_in_dim(starts, block_first, TOK_DEV, 0)
        query_index = block_first + jnp.arange(TOK_DEV, dtype=jnp.int32)
        key_index = block_first - reach_rows + jnp.arange(window_rows, dtype=jnp.int32)
        allowed = (key_index[None, :] >= query_starts[:, None]) & (key_index[None, :] <= query_index[:, None])
        scores = jnp.einsum("thgd,shd->thgs", query_block, key_window) * (HD ** -0.5)
        scores = jnp.where(allowed[:, None, None, :], scores, MASKED_SCORE)
        row_top = jnp.max(scores, axis=-1, keepdims=True)
        weights = jnp.exp(scores - row_top)
        totals = jnp.sum(weights, axis=-1, keepdims=True)
        rounded_weights = lax.optimization_barrier(weights.astype(jnp.bfloat16)).astype(jnp.float32)
        mixed = jnp.einsum("thgs,shd->thgd", rounded_weights, value_window) / totals
        return mixed.reshape(TOK_DEV, HQ * HD).astype(jnp.bfloat16)

    attended = lax.map(one_block, jnp.arange(N_SEQ, dtype=jnp.int32))
    return (attended.reshape(token_count, HQ * HD), rotated_keys)
```

```python
import functools

import jax
import jax.numpy as jnp
import numpy as np
from jax import lax
from jax.experimental import pallas as pl
from jax.experimental.pallas import tpu as pltpu
from jax.sharding import PartitionSpec as P

HD = 128
SPAN = 7
REACH = 4
ROPE_BASE = 1000000.0
SCALE = float(HD ** (-0.5) * np.log2(np.e))
BIG = float(2.0**100)


def rotate(x, cosine, signed_sine):
    x = x.astype(jnp.float32)
    return x * cosine + pltpu.roll(x, HD // 2, 1) * signed_sine


def kernel(
    kv_heads,
    group,
    seg_in,
    q_in,
    k_in,
    v_in,
    table_in,
    freq_in,
    out,
    rk_out,
    segs,
    qraw,
    kv,
    tables,
    freq,
    qt,
    qaug,
    diag,
    own_cos,
    own_sin,
    blk_cos,
    blk_sin,
    kx,
    kaug,
    vt,
    top,
    total,
    acc,
    ovm,
    rkvm,
    in_sem,
    seg_send,
    seg_recv,
    hop_send,
    side_send,
    kv_recv,
    out_sem,
):
    rows = q_in.shape[0]
    half = HD // 2
    me = lax.axis_index("seq")
    n = lax.axis_size("seq")
    core = lax.rem(me, 2)
    own_slot = 1 - core

    def device(offset):
        return {"seq": lax.rem(me + offset + n, n)}

    seg_load = pltpu.make_async_copy(seg_in, segs.at[0], in_sem.at[0])
    seg_load.start()
    kv_loads = []
    for h in range(kv_heads):
        cols = slice(h * HD, (h + 1) * HD)
        for w, src in ((0, k_in), (1, v_in)):
            load = pltpu.make_async_copy(
                src.at[:, cols], kv.at[own_slot, h, w], in_sem.at[4 + 2 * h + w]
            )
            load.start()
            kv_loads.append(load)
    freq_load = pltpu.make_async_copy(freq_in, freq, in_sem.at[1])
    freq_load.start()
    table_load = pltpu.make_async_copy(table_in, tables, in_sem.at[2])
    table_load.start()
    q_load = pltpu.make_async_copy(q_in, qraw, in_sem.at[3])
    q_load.start()

    barrier = pltpu.get_barrier_semaphore()
    for o in range(1, SPAN + 1):
        pl.semaphore_signal(barrier, 1, device_id=device(o))
        pl.semaphore_signal(barrier, 1, device_id=device(-o))
    pl.semaphore_wait(barrier, 2 * SPAN)

    seg_load.wait()
    seg_copies = []
    for o in range(1, SPAN + 1):
        copy = pltpu.make_async_remote_copy(
            src_ref=segs.at[0],
            dst_ref=segs.at[o],
            send_sem=seg_send.at[o - 1],
            recv_sem=seg_recv.at[o - 1],
            device_id=device(o),
        )
        copy.start()
        seg_copies.append(copy)

    def hop(slot, j, h):
        return pltpu.make_async_remote_copy(
            src_ref=kv.at[slot, h],
            dst_ref=kv.at[slot + 2, h],
            send_sem=hop_send.at[j, h],
            recv_sem=kv_recv.at[slot + 2, h],
            device_id=device(2),
        )

    def last_hop(slot, h):
        return pltpu.make_async_remote_copy(
            src_ref=kv.at[slot, h],
            dst_ref=kv.at[slot + 2, h],
            send_sem=hop_send.at[REACH - 1, h],
            recv_sem=kv_recv.at[slot + 2, h],
            device_id=device(1),
        )

    def side(slot, j, h):
        return pltpu.make_async_remote_copy(
            src_ref=kv.at[slot, h],
            dst_ref=kv.at[slot, h],
            send_sem=side_send.at[j, h],
            recv_sem=kv_recv.at[slot, h],
            device_id=device(1 - 2 * core),
        )

    for h in range(kv_heads):
        kv_loads[2 * h].wait()
        kv_loads[2 * h + 1].wait()
        hop(own_slot, 0, h).start()

        @pl.when(core == 0)
        def _():
            side(own_slot, 0, h).start()

    freq_load.wait()
    table_load.wait()
    lane = lax.broadcasted_iota(jnp.int32, (rows, HD), 1)
    sublane = lax.broadcasted_iota(jnp.int32, (rows, HD), 0).astype(jnp.float32)
    sign = jnp.where(lane < half, -1.0, 1.0)
    freq_row = freq[...]
    seg_row = segs[0]
    seg_first = seg_row[:, :1]
    first_row = seg_row == seg_first
    seg_wide = jnp.broadcast_to(seg_row.astype(jnp.float32), (rows, rows))
    seg_tall = seg_wide.T
    key_at = lax.broadcasted_iota(jnp.int32, (rows, rows), 0)
    row_at = lax.broadcasted_iota(jnp.int32, (rows, rows), 1)
    same = seg_tall == seg_wide
    diag[...] = jnp.where(same & (key_at <= row_at), 0.0, -BIG)
    local_position = jnp.sum(
        jnp.where(same & (row_at < key_at), 1.0, 0.0), axis=1, keepdims=True
    )
    first_tall = seg_tall[:, :HD] == seg_first.astype(jnp.float32)
    local_angle = local_position * freq_row
    local_cos = jnp.cos(local_angle)
    local_sin = jnp.sin(local_angle)
    aug_at = lax.broadcasted_iota(jnp.int32, (HD, rows), 0)
    qaug[...] = jnp.where(aug_at == 0, -BIG, 0.0).astype(jnp.bfloat16)

    for copy in seg_copies:
        copy.wait_recv()
    hits = jnp.zeros_like(seg_row, jnp.float32)
    for o in range(1, SPAN + 1):
        hits += jnp.where(segs[o] == seg_first, 1.0, 0.0)
    before = jnp.sum(hits, axis=1, keepdims=True)
    base_angle = before * freq_row
    base_cos = jnp.where(first_tall, jnp.cos(base_angle), 1.0)
    base_sin = jnp.where(first_tall, jnp.sin(base_angle), 0.0)
    own_cos[...] = local_cos * base_cos - local_sin * base_sin
    own_sin[...] = (local_sin * base_cos + local_cos * base_sin) * sign

    for h in range(kv_heads):
        rkvm[:, h * HD : (h + 1) * HD] = rotate(
            kv[own_slot, h, 0], own_cos[...], own_sin[...]
        ).astype(jnp.bfloat16)
    rk_store = pltpu.make_async_copy(rkvm, rk_out, in_sem.at[0])
    rk_store.start()

    q_load.wait()

    def turn(t, carry):
        at = pl.multiple_of(t * HD, HD)
        turned = rotate(qraw[:, pl.ds(at, HD)], own_cos[...], own_sin[...])
        qt[t] = turned.astype(jnp.bfloat16).T
        return carry

    lax.fori_loop(0, kv_heads * group, turn, 0)

    def own_head(h):
        vt[:, :rows] = kv[own_slot, h, 1].T

        def tile(g, carry):
            t = h * group + g
            scores = jnp.dot(
                rkvm[:, h * HD : (h + 1) * HD], qt[t], preferred_element_type=jnp.float32
            )
            scores = scores + diag[...]
            peak = jnp.max(scores, axis=0, keepdims=True)
            weights = jnp.exp2(scores * SCALE - peak * SCALE)
            top[t] = peak
            total[t] = jnp.sum(weights.reshape(rows // 8, 8, rows), axis=0)
            acc[t] = jnp.dot(
                vt[:, :rows], weights.astype(jnp.bfloat16), preferred_element_type=jnp.float32
            )
            return carry

        lax.fori_loop(0, group, tile, 0, unroll=2)

    for h in range(kv_heads):
        own_head(h)

    def prepare(slot, part):
        offset = ((slot - 1 + core) * rows).astype(jnp.float32)
        angle = (before - offset) * freq_row
        c, s = jnp.cos(angle), jnp.sin(angle)
        blk_cos[part] = tables[0] * c - tables[1] * s
        blk_sin[part] = (tables[1] * c + tables[0] * s) * sign
        invalid = (sublane < offset - before) & (lane == 0)
        kaug[part * rows : (part + 1) * rows] = jnp.where(invalid, 1.0, 0.0).astype(jnp.bfloat16)

    def unpack(slot, h, part):
        span = slice(part * rows, (part + 1) * rows)
        kx[span] = rotate(kv[slot, h, 0], blk_cos[part], blk_sin[part]).astype(jnp.bfloat16)
        vt[:, span] = kv[slot, h, 1].T

    def attend(h, depth):
        def tile(g, carry):
            t = h * group + g
            scores = jnp.dot(
                jnp.concatenate([kx[:depth], kaug[:depth]], axis=1),
                jnp.concatenate([qt[t], qaug[...]], axis=0),
                preferred_element_type=jnp.float32,
            )
            old = top[t]
            peak = jnp.where(
                first_row, jnp.maximum(old, jnp.max(scores, axis=0, keepdims=True)), old
            )
            fade = jnp.exp2((old - peak) * SCALE)
            shift = jnp.where(first_row, peak * SCALE, BIG)
            weights = jnp.exp2(scores * SCALE - shift)
            top[t] = peak
            total[t] = total[t] * fade + jnp.sum(
                weights.reshape(depth // 8, 8, rows), axis=0
            )
            acc[t] = acc[t] * fade + jnp.dot(
                vt[:, :depth], weights.astype(jnp.bfloat16), preferred_element_type=jnp.float32
            )
            return carry

        lax.fori_loop(0, group, tile, 0, unroll=2)

    def store(h):
        return pltpu.make_async_copy(
            ovm.at[h], out.at[:, h * group * HD : (h + 1) * group * HD], out_sem.at[h]
        )

    def finish(h):
        for g in range(group):
            t = h * group + g
            share = 1.0 / jnp.sum(total[t], axis=0, keepdims=True)
            ovm[h, :, g * HD : (g + 1) * HD] = (acc[t] * share).astype(jnp.bfloat16).T
        store(h).start()

    @pl.when(core == 1)
    def _():
        prepare(1, 0)
        for h in range(kv_heads):
            side(1, 0, h).wait_recv()
            unpack(1, h, 0)
            attend(h, rows)

    for j in range(1, REACH):
        direct = 2 * j + 1 - core
        other = 2 * j + core
        prepare(direct, 0)
        prepare(other, 1)
        for h in range(kv_heads):
            hop(direct - 2, j - 1, h).wait_recv()
            side(direct, j, h).start()
            if j < REACH - 1:
                hop(direct, j, h).start()
            else:

                @pl.when(core == 1)
                def _():
                    last_hop(direct, h).start()

            unpack(direct, h, 0)
            side(other, j, h).wait_recv()
            unpack(other, h, 1)
            attend(h, 2 * rows)
            if j == REACH - 1:

                @pl.when(core == 1)
                def _():
                    finish(h)

    @pl.when(core == 0)
    def _():
        last = 2 * REACH
        prepare(last, 0)
        for h in range(kv_heads):
            last_hop(last - 2, h).wait_recv()
            unpack(last, h, 0)
            attend(h, rows)
            finish(h)

    for copy in seg_copies:
        copy.wait_send()
    for h in range(kv_heads):
        for j in range(REACH - 1):
            hop(0, j, h).wait_send()
        for j in range(1, REACH):
            side(0, j, h).wait_send()

        @pl.when(core == 0)
        def _():
            side(0, 0, h).wait_send()

        @pl.when(core == 1)
        def _():
            last_hop(0, h).wait_send()

        store(h).wait()
    rk_store.wait()


def local(queries, keys, values, segment_ids):
    rows, width = queries.shape
    kv_width = keys.shape[1]
    heads, kv_heads = width // HD, kv_width // HD
    group = heads // kv_heads
    half = HD // 2
    freq = (ROPE_BASE ** (-(np.arange(half) * (2.0 / HD)))).astype(np.float32)
    freq = np.concatenate([freq, freq])[None]
    angle = (np.arange(rows, dtype=np.float32)[:, None] * freq).astype(np.float64)
    table = np.stack([np.cos(angle), np.sin(angle)]).astype(np.float32)
    any_space = pl.BlockSpec(memory_space=pl.ANY)
    bf16, f32 = jnp.bfloat16, jnp.float32
    slots = 2 * REACH + 1
    dma = pltpu.SemaphoreType.DMA
    return pl.pallas_call(
        functools.partial(kernel, kv_heads, group),
        out_shape=(
            jax.ShapeDtypeStruct((rows, width), bf16),
            jax.ShapeDtypeStruct((rows, kv_width), bf16),
        ),
        in_specs=[any_space] * 6,
        out_specs=(any_space, any_space),
        scratch_shapes=[
            pltpu.VMEM((SPAN + 1, 1, rows), jnp.int32),
            pltpu.VMEM((rows, width), bf16),
            pltpu.VMEM((slots, kv_heads, 2, rows, HD), bf16),
            pltpu.VMEM((2, rows, HD), f32),
            pltpu.VMEM((1, HD), f32),
            pltpu.VMEM((heads, HD, rows), bf16),
            pltpu.VMEM((HD, rows), bf16),
            pltpu.VMEM((rows, rows), f32),
            pltpu.VMEM((rows, HD), f32),
            pltpu.VMEM((rows, HD), f32),
            pltpu.VMEM((2, rows, HD), f32),
            pltpu.VMEM((2, rows, HD), f32),
            pltpu.VMEM((2 * rows, HD), bf16),
            pltpu.VMEM((2 * rows, HD), bf16),
            pltpu.VMEM((HD, 2 * rows), bf16),
            pltpu.VMEM((heads, 1, rows), f32),
            pltpu.VMEM((heads, 8, rows), f32),
            pltpu.VMEM((heads, HD, rows), f32),
            pltpu.VMEM((kv_heads, rows, group * HD), bf16),
            pltpu.VMEM((rows, kv_width), bf16),
            dma((4 + 2 * kv_heads,)),
            dma((SPAN,)),
            dma((SPAN,)),
            dma((REACH, kv_heads)),
            dma((REACH, kv_heads)),
            dma((slots, kv_heads)),
            dma((kv_heads,)),
        ],
        compiler_params=pltpu.CompilerParams(
            collective_id=0, has_side_effects=True, vmem_limit_bytes=56 * 1024 * 1024
        ),
    )(
        segment_ids.reshape(1, rows),
        queries,
        keys,
        values,
        jnp.asarray(table),
        jnp.asarray(freq),
    )


def solution(mesh):
    both = ("groups", "seq")
    return jax.shard_map(
        local,
        mesh=mesh,
        in_specs=(P(both, None), P(both, None), P(both, None), P(both)),
        out_specs=(P(both, None), P(both, None)),
        check_vma=False,
    )
```

```python
import functools

import jax
import jax.numpy as jnp
import numpy as np
from jax import lax
from jax.experimental import pallas as pl
from jax.experimental.pallas import tpu as pltpu
from jax.sharding import PartitionSpec as P

HD = 128
SPAN = 7
REACH = 4
WIDE = 2
ROPE_BASE = 1000000.0
SCALE = float(HD ** (-0.5) * np.log2(np.e))
BIG = float(2.0**100)


def rotate(x, cosine, signed_sine):
    x = x.astype(jnp.float32)
    return x * cosine + pltpu.roll(x, HD // 2, 1) * signed_sine


def kernel(
    kv_heads,
    group,
    seg_in,
    q_in,
    k_in,
    v_in,
    table_in,
    freq_in,
    out,
    rk_out,
    segs,
    qraw,
    kv,
    tables,
    freq,
    qt,
    qaug,
    diag,
    own_cos,
    own_sin,
    blk_cos,
    blk_sin,
    kx,
    kaug,
    vt,
    top,
    total,
    acc,
    raw,
    peaks,
    rounded,
    fades,
    ovm,
    rkvm,
    in_sem,
    seg_send,
    seg_recv,
    hop_send,
    side_send,
    kv_recv,
    out_sem,
):
    rows = q_in.shape[0]
    half = HD // 2
    me = lax.axis_index("seq")
    n = lax.axis_size("seq")
    core = lax.rem(me, 2)
    own_slot = 1 - core

    def device(offset):
        return {"seq": lax.rem(me + offset + n, n)}

    seg_load = pltpu.make_async_copy(seg_in, segs.at[0], in_sem.at[0])
    seg_load.start()
    kv_loads = []
    for h in range(kv_heads):
        cols = slice(h * HD, (h + 1) * HD)
        for w, src in ((0, k_in), (1, v_in)):
            load = pltpu.make_async_copy(
                src.at[:, cols], kv.at[own_slot, h, w], in_sem.at[4 + 2 * h + w]
            )
            load.start()
            kv_loads.append(load)
    freq_load = pltpu.make_async_copy(freq_in, freq, in_sem.at[1])
    freq_load.start()
    table_load = pltpu.make_async_copy(table_in, tables, in_sem.at[2])
    table_load.start()
    q_load = pltpu.make_async_copy(q_in, qraw, in_sem.at[3])
    q_load.start()

    barrier = pltpu.get_barrier_semaphore()
    for o in range(1, SPAN + 1):
        pl.semaphore_signal(barrier, 1, device_id=device(o))
        pl.semaphore_signal(barrier, 1, device_id=device(-o))
    pl.semaphore_wait(barrier, 2 * SPAN)

    seg_load.wait()
    seg_copies = []
    for o in range(1, SPAN + 1):
        copy = pltpu.make_async_remote_copy(
            src_ref=segs.at[0],
            dst_ref=segs.at[o],
            send_sem=seg_send.at[o - 1],
            recv_sem=seg_recv.at[o - 1],
            device_id=device(o),
        )
        copy.start()
        seg_copies.append(copy)

    def hop(slot, j, h):
        return pltpu.make_async_remote_copy(
            src_ref=kv.at[slot, h],
            dst_ref=kv.at[slot + 2, h],
            send_sem=hop_send.at[j, h],
            recv_sem=kv_recv.at[slot + 2, h],
            device_id=device(2),
        )

    def last_hop(slot, h):
        return pltpu.make_async_remote_copy(
            src_ref=kv.at[slot, h],
            dst_ref=kv.at[slot + 2, h],
            send_sem=hop_send.at[REACH - 1, h],
            recv_sem=kv_recv.at[slot + 2, h],
            device_id=device(1),
        )

    def side(slot, j, h):
        return pltpu.make_async_remote_copy(
            src_ref=kv.at[slot, h],
            dst_ref=kv.at[slot, h],
            send_sem=side_send.at[j, h],
            recv_sem=kv_recv.at[slot, h],
            device_id=device(1 - 2 * core),
        )

    for h in range(kv_heads):
        kv_loads[2 * h].wait()
        kv_loads[2 * h + 1].wait()
        hop(own_slot, 0, h).start()

        @pl.when(core == 0)
        def _():
            side(own_slot, 0, h).start()

    freq_load.wait()
    table_load.wait()
    lane = lax.broadcasted_iota(jnp.int32, (rows, HD), 1)
    sublane = lax.broadcasted_iota(jnp.int32, (rows, HD), 0).astype(jnp.float32)
    sign = jnp.where(lane < half, -1.0, 1.0)
    freq_row = freq[...]
    seg_row = segs[0]
    seg_first = seg_row[:, :1]
    first_row = seg_row == seg_first
    seg_wide = jnp.broadcast_to(seg_row.astype(jnp.float32), (rows, rows))
    seg_tall = seg_wide.T
    key_at = lax.broadcasted_iota(jnp.int32, (rows, rows), 0)
    row_at = lax.broadcasted_iota(jnp.int32, (rows, rows), 1)
    same = seg_tall == seg_wide
    diag[...] = jnp.where(same & (key_at <= row_at), 0.0, -BIG)
    local_position = jnp.sum(
        jnp.where(same & (row_at < key_at), 1.0, 0.0), axis=1, keepdims=True
    )
    first_tall = seg_tall[:, :HD] == seg_first.astype(jnp.float32)
    local_angle = local_position * freq_row
    local_cos = jnp.cos(local_angle)
    local_sin = jnp.sin(local_angle)
    aug_at = lax.broadcasted_iota(jnp.int32, (HD, rows), 0)
    later_row = jnp.where(first_row, 0.0, -BIG)
    qaug[...] = jnp.where(
        aug_at == 0, -BIG, jnp.where(aug_at == 1, later_row, 0.0)
    ).astype(jnp.bfloat16)

    def clear(t, carry):
        top[t] = jnp.full((1, rows), -4.0 * BIG, jnp.float32)
        total[t] = jnp.zeros((8, rows), jnp.float32)
        acc[t] = jnp.zeros((HD, rows), jnp.float32)
        return carry

    lax.fori_loop(0, kv_heads * group, clear, 0)

    for copy in seg_copies:
        copy.wait_recv()
    hits = jnp.zeros_like(seg_row, jnp.float32)
    for o in range(1, SPAN + 1):
        hits += jnp.where(segs[o] == seg_first, 1.0, 0.0)
    before = jnp.sum(hits, axis=1, keepdims=True)
    base_angle = before * freq_row
    base_cos = jnp.where(first_tall, jnp.cos(base_angle), 1.0)
    base_sin = jnp.where(first_tall, jnp.sin(base_angle), 0.0)
    own_cos[...] = local_cos * base_cos - local_sin * base_sin
    own_sin[...] = (local_sin * base_cos + local_cos * base_sin) * sign

    for h in range(kv_heads):
        rkvm[:, h * HD : (h + 1) * HD] = rotate(
            kv[own_slot, h, 0], own_cos[...], own_sin[...]
        ).astype(jnp.bfloat16)
    rk_store = pltpu.make_async_copy(rkvm, rk_out, in_sem.at[0])
    rk_store.start()

    q_load.wait()

    def turn(t, carry):
        at = pl.multiple_of(t * HD, HD)
        turned = rotate(qraw[:, pl.ds(at, HD)], own_cos[...], own_sin[...])
        qt[t] = turned.astype(jnp.bfloat16).T
        return carry

    lax.fori_loop(0, kv_heads * group, turn, 0)

    wide_rows = 2 * rows
    per_chunk = group // WIDE
    per_pair = kv_heads * per_chunk
    steps = (SPAN + 1) // 2 * per_pair

    def prepare(pair):
        for part in range(2):
            offset = 2 * pair + part
            distance = (offset * rows).astype(jnp.float32)
            angle = (before - distance) * freq_row
            c, s = jnp.cos(angle), jnp.sin(angle)
            own = offset == 0

            @pl.when(own)
            def _():
                blk_cos[part] = own_cos[...]
                blk_sin[part] = own_sin[...]

            @pl.when(jnp.logical_not(own))
            def _():
                blk_cos[part] = tables[0] * c - tables[1] * s
                blk_sin[part] = (tables[1] * c + tables[0] * s) * sign

            earlier = jnp.where(own, 0.0, 1.0)
            invalid = (sublane < distance - before) & (lane == 0)
            kaug[part * rows : (part + 1) * rows] = jnp.where(
                invalid, 1.0, jnp.where(lane == 1, earlier, 0.0)
            ).astype(jnp.bfloat16)

    def unpack(slot, h, part, buf):
        span = slice(part * rows, (part + 1) * rows)
        kx[buf, span] = rotate(kv[slot, h, 0], blk_cos[part], blk_sin[part]).astype(jnp.bfloat16)
        vt[buf, :, span] = kv[slot, h, 1].T

    def chunk(q):
        pair, h = q // kv_heads, lax.rem(q, kv_heads)
        buf = lax.rem(q, 2)
        ahead = 2 * pair + 3 - core

        @pl.when(pair < REACH - 1)
        def _():
            hop(ahead - 2, pair, h).wait_recv()
            side(ahead, pair + 1, h).start()

        @pl.when(pair < REACH - 2)
        def _():
            hop(ahead, pair + 1, h).start()

        @pl.when((pair == REACH - 2) & (core == 1))
        def _():
            last_hop(ahead, h).start()

        @pl.when(h == 0)
        def _():
            prepare(pair)

        unpack(2 * pair + 1 - core, h, 0, buf)
        other = 2 * pair + 2 - core
        side(other, 0, h).wait_recv()
        unpack(other, h, 1, buf)

    def score(s, own):
        buf = lax.rem(s // per_chunk, 2)
        for u in range(WIDE):
            t = lax.rem(s, per_pair) * WIDE + u
            scores = jnp.dot(
                jnp.concatenate([kx[buf], kaug[...]], axis=1),
                jnp.concatenate([qt[t], qaug[...]], axis=0),
                preferred_element_type=jnp.float32,
            )
            low, high = scores[:rows], scores[rows:]
            if own:
                low = low + diag[...]
            raw[u, :rows] = low
            raw[u, rows:] = high
            peaks[u] = jnp.maximum(
                jnp.max(low.reshape(rows // 8, 8, rows), axis=0),
                jnp.max(high.reshape(rows // 8, 8, rows), axis=0),
            )

    def weigh(s):
        for u in range(WIDE):
            t = lax.rem(s, per_pair) * WIDE + u
            old = top[t]
            peak = jnp.maximum(old, jnp.max(peaks[u], axis=0, keepdims=True))
            fade = jnp.exp2((old - peak) * SCALE)
            weights = jnp.exp2(raw[u] * SCALE - peak * SCALE)
            top[t] = peak
            total[t] = total[t] * fade + jnp.sum(
                weights.reshape(wide_rows // 8, 8, rows), axis=0
            )
            rounded[u] = weights.astype(jnp.bfloat16)
            fades[u] = fade

    def mix(s):
        buf = lax.rem(s // per_chunk, 2)
        for u in range(WIDE):
            t = lax.rem(s, per_pair) * WIDE + u
            acc[t] = acc[t] * fades[u] + jnp.dot(
                vt[buf], rounded[u], preferred_element_type=jnp.float32
            )

    def store(h):
        at = pl.multiple_of(h * group * HD, group * HD)
        return pltpu.make_async_copy(
            ovm.at[h], out.at[:, pl.ds(at, group * HD)], out_sem.at[h]
        )

    def finish(h):
        for g in range(group):
            t = h * group + g
            share = 1.0 / jnp.sum(total[t], axis=0, keepdims=True)
            ovm[h, :, g * HD : (g + 1) * HD] = (acc[t] * share).astype(jnp.bfloat16).T
        store(h).start()

    def step(s, own):
        @pl.when(lax.rem(s, per_chunk) == 0)
        def _():
            chunk(s // per_chunk)

        mix(s - 2)
        weigh(s - 1)
        score(s, own)

    chunk(jnp.int32(0))
    score(jnp.int32(0), True)
    if per_chunk == 1:
        chunk(jnp.int32(1))
    weigh(jnp.int32(0))
    score(jnp.int32(1), True)

    def own_step(s, carry):
        step(s, True)
        return carry

    lax.fori_loop(2, per_pair, own_step, 0)

    def later_step(s, carry):
        ready = s - 2 - (steps - per_pair)

        @pl.when((ready > 0) & (lax.rem(ready, per_chunk) == 0))
        def _():
            finish(ready // per_chunk - 1)

        step(s, False)
        return carry

    lax.fori_loop(per_pair, steps, later_step, 0)
    mix(jnp.int32(steps - 2))
    weigh(jnp.int32(steps - 1))
    for h in range(kv_heads - 1, kv_heads):
        mix(jnp.int32(steps - 1))
        finish(h)

    for copy in seg_copies:
        copy.wait_send()
    for h in range(kv_heads):
        for j in range(REACH - 1):
            hop(0, j, h).wait_send()
        for j in range(1, REACH):
            side(0, j, h).wait_send()

        @pl.when(core == 0)
        def _():
            side(0, 0, h).wait_send()

        @pl.when(core == 1)
        def _():
            last_hop(0, h).wait_send()

        store(h).wait()
    rk_store.wait()


def local(queries, keys, values, segment_ids):
    rows, width = queries.shape
    kv_width = keys.shape[1]
    heads, kv_heads = width // HD, kv_width // HD
    group = heads // kv_heads
    half = HD // 2
    freq = (ROPE_BASE ** (-(np.arange(half) * (2.0 / HD)))).astype(np.float32)
    freq = np.concatenate([freq, freq])[None]
    angle = (np.arange(rows, dtype=np.float32)[:, None] * freq).astype(np.float64)
    table = np.stack([np.cos(angle), np.sin(angle)]).astype(np.float32)
    any_space = pl.BlockSpec(memory_space=pl.ANY)
    bf16, f32 = jnp.bfloat16, jnp.float32
    slots = 2 * REACH + 1
    dma = pltpu.SemaphoreType.DMA
    return pl.pallas_call(
        functools.partial(kernel, kv_heads, group),
        out_shape=(
            jax.ShapeDtypeStruct((rows, width), bf16),
            jax.ShapeDtypeStruct((rows, kv_width), bf16),
        ),
        in_specs=[any_space] * 6,
        out_specs=(any_space, any_space),
        scratch_shapes=[
            pltpu.VMEM((SPAN + 1, 1, rows), jnp.int32),
            pltpu.VMEM((rows, width), bf16),
            pltpu.VMEM((slots, kv_heads, 2, rows, HD), bf16),
            pltpu.VMEM((2, rows, HD), f32),
            pltpu.VMEM((1, HD), f32),
            pltpu.VMEM((heads, HD, rows), bf16),
            pltpu.VMEM((HD, rows), bf16),
            pltpu.VMEM((rows, rows), f32),
            pltpu.VMEM((rows, HD), f32),
            pltpu.VMEM((rows, HD), f32),
            pltpu.VMEM((2, rows, HD), f32),
            pltpu.VMEM((2, rows, HD), f32),
            pltpu.VMEM((2, 2 * rows, HD), bf16),
            pltpu.VMEM((2 * rows, HD), bf16),
            pltpu.VMEM((2, HD, 2 * rows), bf16),
            pltpu.VMEM((heads, 1, rows), f32),
            pltpu.VMEM((heads, 8, rows), f32),
            pltpu.VMEM((heads, HD, rows), f32),
            pltpu.VMEM((WIDE, 2 * rows, rows), f32),
            pltpu.VMEM((WIDE, 8, rows), f32),
            pltpu.VMEM((WIDE, 2 * rows, rows), bf16),
            pltpu.VMEM((WIDE, 1, rows), f32),
            pltpu.VMEM((kv_heads, rows, group * HD), bf16),
            pltpu.VMEM((rows, kv_width), bf16),
            dma((4 + 2 * kv_heads,)),
            dma((SPAN,)),
            dma((SPAN,)),
            dma((REACH, kv_heads)),
            dma((REACH, kv_heads)),
            dma((slots, kv_heads)),
            dma((kv_heads,)),
        ],
        compiler_params=pltpu.CompilerParams(
            collective_id=0, has_side_effects=True, vmem_limit_bytes=56 * 1024 * 1024
        ),
    )(
        segment_ids.reshape(1, rows),
        queries,
        keys,
        values,
        jnp.asarray(table),
        jnp.asarray(freq),
    )


def solution(mesh):
    both = ("groups", "seq")
    return jax.shard_map(
        local,
        mesh=mesh,
        in_specs=(P(both, None), P(both, None), P(both, None), P(both)),
        out_specs=(P(both, None), P(both, None)),
        check_vma=False,
    )
```

```python
import functools
import math

import jax
import jax.numpy as jnp
import numpy as np
from jax import lax
from jax.experimental import pallas as pl
from jax.experimental.pallas import tpu as pltpu
from jax.sharding import PartitionSpec as P

HD = 128
SPAN = 7
REACH = 4
WIDE = 2
TURNED = 2
ROPE_BASE = 1000000.0
SCALE = float(HD ** (-0.5) * np.log2(np.e))
BIG = float(2.0**100)


def rotate(x, cosine, signed_sine):
    x = x.astype(jnp.float32)
    return x * cosine + pltpu.roll(x, HD // 2, 1) * signed_sine


def kernel(
    kv_heads,
    group,
    seg_in,
    q_in,
    k_in,
    v_in,
    table_in,
    freq_in,
    out,
    rk_out,
    segs,
    qraw,
    kv,
    tables,
    freq,
    qt,
    qaug,
    diag,
    own_cos,
    own_sin,
    blk_cos,
    blk_sin,
    kx,
    kaug,
    vt,
    top,
    total,
    acc,
    raw,
    peaks,
    rounded,
    fades,
    ovm,
    rkvm,
    in_sem,
    seg_send,
    seg_recv,
    hop_send,
    side_send,
    chain_send,
    via,
    via_send,
    via_recv,
    leg_send,
    kv_recv,
    out_sem,
):
    rows = q_in.shape[0]
    half = HD // 2
    me = lax.axis_index("seq")
    n = lax.axis_size("seq")
    core = lax.rem(me, 2)
    own_slot = 1 - core
    chip = me // 2
    last = n // 2 - 1
    width = math.isqrt(n // 2)

    def device(offset):
        return {"seq": me + offset}

    def relay_of(source):
        return source // width * width + lax.rem(source + width - 2, width)

    def far_of(source):
        return jnp.minimum(source + REACH, last)

    relayed = chip // width * width + lax.rem(chip + 2, width)

    seg_load = pltpu.make_async_copy(seg_in, segs.at[0], in_sem.at[0])
    seg_load.start()
    kv_loads = []
    for h in range(kv_heads):
        cols = slice(h * HD, (h + 1) * HD)
        for w, src in ((0, k_in), (1, v_in)):
            load = pltpu.make_async_copy(
                src.at[:, cols], kv.at[own_slot, h, w], in_sem.at[4 + 2 * h + w]
            )
            load.start()
            kv_loads.append(load)
    freq_load = pltpu.make_async_copy(freq_in, freq, in_sem.at[1])
    freq_load.start()
    table_load = pltpu.make_async_copy(table_in, tables, in_sem.at[2])
    table_load.start()
    q_load = pltpu.make_async_copy(q_in, qraw, in_sem.at[3])
    q_load.start()

    barrier = pltpu.get_barrier_semaphore()

    def tell(rank, when):
        @pl.when(when)
        def _():
            pl.semaphore_signal(barrier, 1, device_id={"seq": rank})

    for o in range(1, SPAN + 1):
        tell(me - o, me >= o)
    tell(me + 1, (core == 0) & (chip >= 1))
    tell(me + 2, (core == 0) & (chip >= 1) & (chip < last))
    tell(2 * relayed + 1, (core == 1) & (relayed < last))
    tell(2 * relay_of(chip - REACH) + 1, (core == 0) & (chip >= REACH))
    for back in range(1, REACH):
        tell(2 * relay_of(chip - back) + 1, (core == 0) & (chip == last))
    receivers = jnp.minimum(SPAN, n - 1 - me) + jnp.where(
        core == 0,
        jnp.where(chip >= 2, 1, 0),
        jnp.where(chip >= 1, 1, 0)
        + jnp.where(chip < last, 1, 0)
        + jnp.where(relayed < last, 1, 0),
    )
    pl.semaphore_wait(barrier, receivers)

    seg_load.wait()
    def seg_copy(o):
        return pltpu.make_async_remote_copy(
            src_ref=segs.at[0],
            dst_ref=segs.at[o],
            send_sem=seg_send.at[o - 1],
            recv_sem=seg_recv.at[o - 1],
            device_id=device(o),
        )

    for o in range(1, SPAN + 1):

        @pl.when(me + o < n)
        def _():
            seg_copy(o).start()

    def hop(slot, h):
        return pltpu.make_async_remote_copy(
            src_ref=kv.at[slot, h],
            dst_ref=kv.at[slot + 2, h],
            send_sem=hop_send.at[slot, h],
            recv_sem=kv_recv.at[slot + 2, h],
            device_id=device(2),
        )

    def last_hop(slot, h):
        return pltpu.make_async_remote_copy(
            src_ref=kv.at[slot, h],
            dst_ref=kv.at[slot + 2, h],
            send_sem=hop_send.at[slot, h],
            recv_sem=kv_recv.at[slot + 2, h],
            device_id=device(1),
        )

    def side(slot, h):
        return pltpu.make_async_remote_copy(
            src_ref=kv.at[slot, h],
            dst_ref=kv.at[slot, h],
            send_sem=side_send.at[slot, h],
            recv_sem=kv_recv.at[slot, h],
            device_id=device(1 - 2 * core),
        )

    def back_hop(slot, h):
        return pltpu.make_async_remote_copy(
            src_ref=kv.at[slot, h],
            dst_ref=kv.at[slot - 2, h],
            send_sem=chain_send.at[slot, h],
            recv_sem=kv_recv.at[slot - 2, h],
            device_id=device(-2),
        )

    def first_leg(h):
        return pltpu.make_async_remote_copy(
            src_ref=kv.at[own_slot, h],
            dst_ref=via.at[h - TURNED],
            send_sem=via_send.at[h - TURNED],
            recv_sem=via_recv.at[h - TURNED],
            device_id={"seq": 2 * relay_of(chip) + 1},
        )

    def second_leg(h):
        far = far_of(relayed)
        slot = 2 * (far - relayed)
        return pltpu.make_async_remote_copy(
            src_ref=via.at[h - TURNED],
            dst_ref=kv.at[slot, h],
            send_sem=leg_send.at[h - TURNED],
            recv_sem=kv_recv.at[slot, h],
            device_id={"seq": 2 * far},
        )

    for h in range(kv_heads):
        kv_loads[2 * h].wait()
        kv_loads[2 * h + 1].wait()

        @pl.when((chip < last) & ((core == 0) | (h < TURNED)))
        def _():
            hop(own_slot, h).start()

        if h >= TURNED:

            @pl.when((chip < last) & (core == 1))
            def _():
                first_leg(h).start()

        @pl.when(core == 0)
        def _():
            side(own_slot, h).start()

    def blank(slot, carry):
        @pl.when(chip < slot // 2)
        def _():
            kv[slot] = jnp.zeros(kv.shape[1:], kv.dtype)

        return carry

    lax.fori_loop(2, 2 * REACH + 1, blank, 0)

    freq_load.wait()
    table_load.wait()
    lane = lax.broadcasted_iota(jnp.int32, (rows, HD), 1)
    sublane = lax.broadcasted_iota(jnp.int32, (rows, HD), 0).astype(jnp.float32)
    sign = jnp.where(lane < half, -1.0, 1.0)
    freq_row = freq[...]
    seg_row = segs[0]
    seg_first = seg_row[:, :1]
    first_row = seg_row == seg_first
    seg_wide = jnp.broadcast_to(seg_row.astype(jnp.float32), (rows, rows))
    seg_tall = seg_wide.T
    key_at = lax.broadcasted_iota(jnp.int32, (rows, rows), 0)
    row_at = lax.broadcasted_iota(jnp.int32, (rows, rows), 1)
    same = seg_tall == seg_wide
    diag[...] = jnp.where(same & (key_at <= row_at), 0.0, -BIG)
    local_position = jnp.sum(
        jnp.where(same & (row_at < key_at), 1.0, 0.0), axis=1, keepdims=True
    )
    first_tall = seg_tall[:, :HD] == seg_first.astype(jnp.float32)
    local_angle = local_position * freq_row
    local_cos = jnp.cos(local_angle)
    local_sin = jnp.sin(local_angle)
    aug_at = lax.broadcasted_iota(jnp.int32, (HD, rows), 0)
    later_row = jnp.where(first_row, 0.0, -BIG)
    qaug[...] = jnp.where(
        aug_at == 0, -BIG, jnp.where(aug_at == 1, later_row, 0.0)
    ).astype(jnp.bfloat16)

    def clear(t, carry):
        top[t] = jnp.full((1, rows), -4.0 * BIG, jnp.float32)
        total[t] = jnp.zeros((8, rows), jnp.float32)
        acc[t] = jnp.zeros((HD, rows), jnp.float32)
        return carry

    lax.fori_loop(0, kv_heads * group, clear, 0)

    for o in range(1, SPAN + 1):

        @pl.when(me >= o)
        def _():
            seg_copy(o).wait_recv()

        @pl.when(me < o)
        def _():
            segs[o] = jnp.full((1, rows), -1, jnp.int32)

    hits = jnp.zeros_like(seg_row, jnp.float32)
    for o in range(1, SPAN + 1):
        hits += jnp.where(segs[o] == seg_first, 1.0, 0.0)
    before = jnp.sum(hits, axis=1, keepdims=True)
    base_angle = before * freq_row
    base_cos = jnp.where(first_tall, jnp.cos(base_angle), 1.0)
    base_sin = jnp.where(first_tall, jnp.sin(base_angle), 0.0)
    own_cos[...] = local_cos * base_cos - local_sin * base_sin
    own_sin[...] = (local_sin * base_cos + local_cos * base_sin) * sign

    for h in range(kv_heads):
        rkvm[:, h * HD : (h + 1) * HD] = rotate(
            kv[own_slot, h, 0], own_cos[...], own_sin[...]
        ).astype(jnp.bfloat16)
    rk_store = pltpu.make_async_copy(rkvm, rk_out, in_sem.at[0])
    rk_store.start()

    q_load.wait()

    def turn(t, carry):
        at = pl.multiple_of(t * HD, HD)
        turned = rotate(qraw[:, pl.ds(at, HD)], own_cos[...], own_sin[...])
        qt[t] = turned.astype(jnp.bfloat16).T
        return carry

    lax.fori_loop(0, kv_heads * group, turn, 0)

    wide_rows = 2 * rows
    per_chunk = group // WIDE
    per_pair = kv_heads * per_chunk
    steps = (SPAN + 1) // 2 * per_pair

    def prepare(pair, slots):
        for part, slot in enumerate(slots):
            offset = slot - 1 + core
            distance = (offset * rows).astype(jnp.float32)
            angle = (before - distance) * freq_row
            c, s = jnp.cos(angle), jnp.sin(angle)
            own = offset == 0

            @pl.when(own)
            def _():
                blk_cos[part] = own_cos[...]
                blk_sin[part] = own_sin[...]

            @pl.when(jnp.logical_not(own))
            def _():
                blk_cos[part] = tables[0] * c - tables[1] * s
                blk_sin[part] = (tables[1] * c + tables[0] * s) * sign

            earlier = jnp.where(own, 0.0, 1.0)
            invalid = (sublane < distance - before) & (lane == 0)
            kaug[part * rows : (part + 1) * rows] = jnp.where(
                invalid, 1.0, jnp.where(lane == 1, earlier, 0.0)
            ).astype(jnp.bfloat16)

    def unpack(slot, h, part, buf):
        span = slice(part * rows, (part + 1) * rows)
        kx[buf, span] = rotate(kv[slot, h, 0], blk_cos[part], blk_sin[part]).astype(jnp.bfloat16)
        vt[buf, :, span] = kv[slot, h, 1].T

    def chunk(q):
        pair, h = q // kv_heads, lax.rem(q, kv_heads)
        buf = lax.rem(q, 2)
        forward = h < TURNED
        back = h >= TURNED
        far = REACH - pair

        ahead = 2 * pair + 3 - core
        mine = (pair < REACH - 1) & (chip >= pair + 1) & ((core == 0) | forward)

        @pl.when(mine)
        def _():
            hop(ahead - 2, h).wait_recv()
            side(ahead, h).start()

        @pl.when(mine & (chip < last) & (pair < REACH - 2))
        def _():
            hop(ahead, h).start()

        @pl.when(mine & (chip < last) & (pair == REACH - 2) & (core == 1))
        def _():
            last_hop(ahead, h).start()

        @pl.when(back & (pair == 0) & (core == 1) & (relayed < last))
        def _():
            first_leg(h).wait_recv()
            second_leg(h).start()

        chained = back & (core == 0) & (chip >= far)

        @pl.when(chained)
        def _():
            side(2 * far, h).wait_recv()

        @pl.when(chained & (far >= 2))
        def _():
            back_hop(2 * far, h).start()

        @pl.when(chained & (far < REACH))
        def _():
            side(2 * far, h).start()

        one = jnp.where(forward | (pair == 0), 2 * pair + 1 - core, 2 * pair + 1)
        two = jnp.where(
            forward, 2 * pair + 2 - core, jnp.where((pair == 0) & (core == 1), 1, 2 * far)
        )

        @pl.when((h == 0) | (h == TURNED))
        def _():
            prepare(pair, (one, two))

        @pl.when(back & (pair > 0) & (core == 1) & (chip >= pair))
        def _():
            side(one, h).wait_recv()

        unpack(one, h, 0, buf)

        @pl.when((chip >= two // 2) & (forward | (core == 1)))
        def _():
            side(two, h).wait_recv()

        unpack(two, h, 1, buf)

    def score(s, own):
        buf = lax.rem(s // per_chunk, 2)
        for u in range(WIDE):
            t = lax.rem(s, per_pair) * WIDE + u
            scores = jnp.dot(
                jnp.concatenate([kx[buf], kaug[...]], axis=1),
                jnp.concatenate([qt[t], qaug[...]], axis=0),
                preferred_element_type=jnp.float32,
            )
            low, high = scores[:rows], scores[rows:]
            if own:
                low = low + diag[...]
            raw[u, :rows] = low
            raw[u, rows:] = high
            peaks[u] = jnp.maximum(
                jnp.max(low.reshape(rows // 8, 8, rows), axis=0),
                jnp.max(high.reshape(rows // 8, 8, rows), axis=0),
            )

    def weigh(s):
        for u in range(WIDE):
            t = lax.rem(s, per_pair) * WIDE + u
            old = top[t]
            peak = jnp.maximum(old, jnp.max(peaks[u], axis=0, keepdims=True))
            fade = jnp.exp2((old - peak) * SCALE)
            weights = jnp.exp2(raw[u] * SCALE - peak * SCALE)
            top[t] = peak
            total[t] = total[t] * fade + jnp.sum(
                weights.reshape(wide_rows // 8, 8, rows), axis=0
            )
            rounded[u] = weights.astype(jnp.bfloat16)
            fades[u] = fade

    def mix(s):
        buf = lax.rem(s // per_chunk, 2)
        for u in range(WIDE):
            t = lax.rem(s, per_pair) * WIDE + u
            acc[t] = acc[t] * fades[u] + jnp.dot(
                vt[buf], rounded[u], preferred_element_type=jnp.float32
            )

    def store(h):
        at = pl.multiple_of(h * group * HD, group * HD)
        return pltpu.make_async_copy(
            ovm.at[h], out.at[:, pl.ds(at, group * HD)], out_sem.at[h]
        )

    def finish(h):
        for g in range(group):
            t = h * group + g
            share = 1.0 / jnp.sum(total[t], axis=0, keepdims=True)
            ovm[h, :, g * HD : (g + 1) * HD] = (acc[t] * share).astype(jnp.bfloat16).T
        store(h).start()

    def step(s, own):
        @pl.when(lax.rem(s, per_chunk) == 0)
        def _():
            chunk(s // per_chunk)

        mix(s - 2)
        weigh(s - 1)
        score(s, own)

    chunk(jnp.int32(0))
    score(jnp.int32(0), True)
    if per_chunk == 1:
        chunk(jnp.int32(1))
    weigh(jnp.int32(0))
    score(jnp.int32(1), True)

    def own_step(s, carry):
        step(s, True)
        return carry

    lax.fori_loop(2, per_pair, own_step, 0)

    def later_step(s, carry):
        ready = s - 2 - (steps - per_pair)

        @pl.when((ready > 0) & (lax.rem(ready, per_chunk) == 0))
        def _():
            finish(ready // per_chunk - 1)

        step(s, False)
        return carry

    lax.fori_loop(per_pair, steps, later_step, 0)
    mix(jnp.int32(steps - 2))
    weigh(jnp.int32(steps - 1))
    for h in range(kv_heads - 1, kv_heads):
        mix(jnp.int32(steps - 1))
        finish(h)

    def drain(copy, when):
        @pl.when(when)
        def _():
            copy.wait_send()

    for o in range(1, SPAN + 1):
        drain(seg_copy(o), me + o < n)
    for h in range(kv_heads):
        lane_here = (core == 0) | (h < TURNED)
        for j in range(REACH):
            slot = 2 * j + own_slot
            sends = lane_here & (chip >= j) & (chip < last)
            if j == REACH - 1:
                sends = sends & (core == 1)
            drain(hop(slot, h), sends)
            drain(side(slot, h), (lane_here & (chip >= j)) if j else core == 0)
        if h >= TURNED:
            drain(first_leg(h), (core == 1) & (chip < last))
            drain(second_leg(h), (core == 1) & (relayed < last))
            for j in range(1, REACH + 1):
                turned = (core == 0) & (chip >= j)
                if j >= 2:
                    drain(back_hop(2 * j, h), turned)
                if j < REACH:
                    drain(side(2 * j, h), turned)
        store(h).wait()
    rk_store.wait()


def local(queries, keys, values, segment_ids):
    rows, width = queries.shape
    kv_width = keys.shape[1]
    heads, kv_heads = width // HD, kv_width // HD
    group = heads // kv_heads
    half = HD // 2
    freq = (ROPE_BASE ** (-(np.arange(half) * (2.0 / HD)))).astype(np.float32)
    freq = np.concatenate([freq, freq])[None]
    angle = (np.arange(rows, dtype=np.float32)[:, None] * freq).astype(np.float64)
    table = np.stack([np.cos(angle), np.sin(angle)]).astype(np.float32)
    any_space = pl.BlockSpec(memory_space=pl.ANY)
    bf16, f32 = jnp.bfloat16, jnp.float32
    slots = 2 * REACH + 1
    dma = pltpu.SemaphoreType.DMA
    return pl.pallas_call(
        functools.partial(kernel, kv_heads, group),
        out_shape=(
            jax.ShapeDtypeStruct((rows, width), bf16),
            jax.ShapeDtypeStruct((rows, kv_width), bf16),
        ),
        in_specs=[any_space] * 6,
        out_specs=(any_space, any_space),
        scratch_shapes=[
            pltpu.VMEM((SPAN + 1, 1, rows), jnp.int32),
            pltpu.VMEM((rows, width), bf16),
            pltpu.VMEM((slots, kv_heads, 2, rows, HD), bf16),
            pltpu.VMEM((2, rows, HD), f32),
            pltpu.VMEM((1, HD), f32),
            pltpu.VMEM((heads, HD, rows), bf16),
            pltpu.VMEM((HD, rows), bf16),
            pltpu.VMEM((rows, rows), f32),
            pltpu.VMEM((rows, HD), f32),
            pltpu.VMEM((rows, HD), f32),
            pltpu.VMEM((2, rows, HD), f32),
            pltpu.VMEM((2, rows, HD), f32),
            pltpu.VMEM((2, 2 * rows, HD), bf16),
            pltpu.VMEM((2 * rows, HD), bf16),
            pltpu.VMEM((2, HD, 2 * rows), bf16),
            pltpu.VMEM((heads, 1, rows), f32),
            pltpu.VMEM((heads, 8, rows), f32),
            pltpu.VMEM((heads, HD, rows), f32),
            pltpu.VMEM((WIDE, 2 * rows, rows), f32),
            pltpu.VMEM((WIDE, 8, rows), f32),
            pltpu.VMEM((WIDE, 2 * rows, rows), bf16),
            pltpu.VMEM((WIDE, 1, rows), f32),
            pltpu.VMEM((kv_heads, rows, group * HD), bf16),
            pltpu.VMEM((rows, kv_width), bf16),
            dma((4 + 2 * kv_heads,)),
            dma((SPAN,)),
            dma((SPAN,)),
            dma((slots, kv_heads)),
            dma((slots, kv_heads)),
            dma((slots, kv_heads)),
            pltpu.VMEM((kv_heads - TURNED, 2, rows, HD), bf16),
            dma((kv_heads - TURNED,)),
            dma((kv_heads - TURNED,)),
            dma((kv_heads - TURNED,)),
            dma((slots, kv_heads)),
            dma((kv_heads,)),
        ],
        compiler_params=pltpu.CompilerParams(
            collective_id=0, has_side_effects=True, vmem_limit_bytes=56 * 1024 * 1024
        ),
    )(
        segment_ids.reshape(1, rows),
        queries,
        keys,
        values,
        jnp.asarray(table),
        jnp.asarray(freq),
    )


def solution(mesh):
    both = ("groups", "seq")
    return jax.shard_map(
        local,
        mesh=mesh,
        in_specs=(P(both, None), P(both, None), P(both, None), P(both)),
        out_specs=(P(both, None), P(both, None)),
        check_vma=False,
    )
```

```python
import functools
import math

import jax
import jax.numpy as jnp
import numpy as np
from jax import lax
from jax.experimental import pallas as pl
from jax.experimental.pallas import tpu as pltpu
from jax.sharding import PartitionSpec as P

HD = 128
SPAN = 7
REACH = 4
STRIP = 128
TURNED = 2
ROPE_BASE = 1000000.0
SCALE = float(HD ** (-0.5) * np.log2(np.e))
BIG = float(2.0**100)


def rotate(x, cosine, signed_sine):
    x = x.astype(jnp.float32)
    return x * cosine + pltpu.roll(x, HD // 2, 1) * signed_sine


def kernel(
    kv_heads,
    group,
    seg_in,
    q_in,
    k_in,
    v_in,
    table_in,
    freq_in,
    out,
    rk_out,
    segs,
    qraw,
    kv,
    tables,
    freq,
    qt,
    diag,
    own_cos,
    own_sin,
    blk_cos,
    blk_sin,
    kx,
    vt,
    top,
    anchor,
    acc,
    raw,
    peaks,
    ovm,
    rkvm,
    in_sem,
    seg_send,
    seg_recv,
    hop_send,
    side_send,
    chain_send,
    via,
    via_send,
    via_recv,
    leg_send,
    kv_recv,
    out_sem,
):
    rows = q_in.shape[0]
    half = HD // 2
    me = lax.axis_index("seq")
    n = lax.axis_size("seq")
    core = lax.rem(me, 2)
    own_slot = 1 - core
    chip = me // 2
    last = n // 2 - 1
    width = math.isqrt(n // 2)

    def device(offset):
        return {"seq": me + offset}

    def relay_of(source):
        return source // width * width + lax.rem(source + width - 2, width)

    def far_of(source):
        return jnp.minimum(source + REACH, last)

    relayed = chip // width * width + lax.rem(chip + 2, width)

    seg_load = pltpu.make_async_copy(seg_in, segs.at[0], in_sem.at[0])
    seg_load.start()
    kv_loads = []
    for h in range(kv_heads):
        cols = slice(h * HD, (h + 1) * HD)
        for w, src in ((0, k_in), (1, v_in)):
            load = pltpu.make_async_copy(
                src.at[:, cols], kv.at[own_slot, h, w], in_sem.at[4 + 2 * h + w]
            )
            load.start()
            kv_loads.append(load)
    freq_load = pltpu.make_async_copy(freq_in, freq, in_sem.at[1])
    freq_load.start()
    table_load = pltpu.make_async_copy(table_in, tables, in_sem.at[2])
    table_load.start()
    q_load = pltpu.make_async_copy(q_in, qraw, in_sem.at[3])
    q_load.start()

    barrier = pltpu.get_barrier_semaphore()

    def tell(rank, when):
        @pl.when(when)
        def _():
            pl.semaphore_signal(barrier, 1, device_id={"seq": rank})

    for o in range(1, SPAN + 1):
        tell(me - o, me >= o)
    tell(me + 1, (core == 0) & (chip >= 1))
    tell(me + 2, (core == 0) & (chip >= 1) & (chip < last))
    tell(2 * relayed + 1, (core == 1) & (relayed < last))
    tell(2 * relay_of(chip - REACH) + 1, (core == 0) & (chip >= REACH))
    for back in range(1, REACH):
        tell(2 * relay_of(chip - back) + 1, (core == 0) & (chip == last))
    receivers = jnp.minimum(SPAN, n - 1 - me) + jnp.where(
        core == 0,
        jnp.where(chip >= 2, 1, 0),
        jnp.where(chip >= 1, 1, 0)
        + jnp.where(chip < last, 1, 0)
        + jnp.where(relayed < last, 1, 0),
    )
    pl.semaphore_wait(barrier, receivers)

    seg_load.wait()
    def seg_copy(o):
        return pltpu.make_async_remote_copy(
            src_ref=segs.at[0],
            dst_ref=segs.at[o],
            send_sem=seg_send.at[o - 1],
            recv_sem=seg_recv.at[o - 1],
            device_id=device(o),
        )

    for o in range(1, SPAN + 1):

        @pl.when(me + o < n)
        def _():
            seg_copy(o).start()

    def hop(slot, h):
        return pltpu.make_async_remote_copy(
            src_ref=kv.at[slot, h],
            dst_ref=kv.at[slot + 2, h],
            send_sem=hop_send.at[slot, h],
            recv_sem=kv_recv.at[slot + 2, h],
            device_id=device(2),
        )

    def last_hop(slot, h):
        return pltpu.make_async_remote_copy(
            src_ref=kv.at[slot, h],
            dst_ref=kv.at[slot + 2, h],
            send_sem=hop_send.at[slot, h],
            recv_sem=kv_recv.at[slot + 2, h],
            device_id=device(1),
        )

    def side(slot, h):
        return pltpu.make_async_remote_copy(
            src_ref=kv.at[slot, h],
            dst_ref=kv.at[slot, h],
            send_sem=side_send.at[slot, h],
            recv_sem=kv_recv.at[slot, h],
            device_id=device(1 - 2 * core),
        )

    def back_hop(slot, h):
        return pltpu.make_async_remote_copy(
            src_ref=kv.at[slot, h],
            dst_ref=kv.at[slot - 2, h],
            send_sem=chain_send.at[slot, h],
            recv_sem=kv_recv.at[slot - 2, h],
            device_id=device(-2),
        )

    def first_leg(h):
        return pltpu.make_async_remote_copy(
            src_ref=kv.at[own_slot, h],
            dst_ref=via.at[h - TURNED],
            send_sem=via_send.at[h - TURNED],
            recv_sem=via_recv.at[h - TURNED],
            device_id={"seq": 2 * relay_of(chip) + 1},
        )

    def second_leg(h):
        far = far_of(relayed)
        slot = 2 * (far - relayed)
        return pltpu.make_async_remote_copy(
            src_ref=via.at[h - TURNED],
            dst_ref=kv.at[slot, h],
            send_sem=leg_send.at[h - TURNED],
            recv_sem=kv_recv.at[slot, h],
            device_id={"seq": 2 * far},
        )

    for h in range(kv_heads):
        kv_loads[2 * h].wait()
        kv_loads[2 * h + 1].wait()

        @pl.when((chip < last) & ((core == 0) | (h < TURNED)))
        def _():
            hop(own_slot, h).start()

        if h >= TURNED:

            @pl.when((chip < last) & (core == 1))
            def _():
                first_leg(h).start()

        @pl.when(core == 0)
        def _():
            side(own_slot, h).start()

    def blank(slot, carry):
        @pl.when(chip < slot // 2)
        def _():
            kv[slot] = jnp.zeros(kv.shape[1:], kv.dtype)

        return carry

    lax.fori_loop(2, 2 * REACH + 1, blank, 0)

    freq_load.wait()
    table_load.wait()
    lane = lax.broadcasted_iota(jnp.int32, (rows, HD), 1)
    sublane = lax.broadcasted_iota(jnp.int32, (rows, HD), 0).astype(jnp.float32)
    sign = jnp.where(lane < half, -1.0, 1.0)
    freq_row = freq[...]
    seg_row = segs[0]
    seg_first = seg_row[:, :1]
    first_row = seg_row == seg_first
    seg_wide = jnp.broadcast_to(seg_row.astype(jnp.float32), (rows, rows))
    seg_tall = seg_wide.T
    key_at = lax.broadcasted_iota(jnp.int32, (rows, rows), 0)
    row_at = lax.broadcasted_iota(jnp.int32, (rows, rows), 1)
    same = seg_tall == seg_wide
    diag[...] = jnp.where(same & (key_at <= row_at), 0.0, -BIG)
    local_position = jnp.sum(
        jnp.where(same & (row_at < key_at), 1.0, 0.0), axis=1, keepdims=True
    )
    first_tall = seg_tall[:, :HD] == seg_first.astype(jnp.float32)
    local_angle = local_position * freq_row
    local_cos = jnp.cos(local_angle)
    local_sin = jnp.sin(local_angle)
    def clear(t, carry):
        top[t] = jnp.full((1, rows), -4.0 * BIG, jnp.float32)
        acc[t] = jnp.zeros(acc.shape[1:], jnp.float32)
        return carry

    lax.fori_loop(0, kv_heads * group, clear, 0)

    for o in range(1, SPAN + 1):

        @pl.when(me >= o)
        def _():
            seg_copy(o).wait_recv()

        @pl.when(me < o)
        def _():
            segs[o] = jnp.full((1, rows), -1, jnp.int32)

    hits = jnp.zeros_like(seg_row, jnp.float32)
    for o in range(1, SPAN + 1):
        hits += jnp.where(segs[o] == seg_first, 1.0, 0.0)
    before = jnp.sum(hits, axis=1, keepdims=True)
    base_angle = before * freq_row
    base_cos = jnp.where(first_tall, jnp.cos(base_angle), 1.0)
    base_sin = jnp.where(first_tall, jnp.sin(base_angle), 0.0)
    own_cos[...] = local_cos * base_cos - local_sin * base_sin
    own_sin[...] = (local_sin * base_cos + local_cos * base_sin) * sign

    for h in range(kv_heads):
        turned_keys = rotate(kv[own_slot, h, 0], own_cos[...], own_sin[...])
        anchor[h] = turned_keys[:8]
        rkvm[:, h * HD : (h + 1) * HD] = turned_keys.astype(jnp.bfloat16)
    rk_store = pltpu.make_async_copy(rkvm, rk_out, in_sem.at[0])
    rk_store.start()

    q_load.wait()

    def turn(t, carry):
        at = pl.multiple_of(t * HD, HD)
        turned = rotate(qraw[:, pl.ds(at, HD)], own_cos[...], own_sin[...])
        qt[t] = turned.astype(jnp.bfloat16).T
        return carry

    lax.fori_loop(0, kv_heads * group, turn, 0)

    chunks = (SPAN + 1) // 2 * kv_heads
    allowed_row = jnp.where(first_row, 0.0, -BIG)

    def split(q):
        pair = q // kv_heads
        h = lax.rem(q, kv_heads)
        h = jnp.where(pair == REACH - 1, lax.rem(h + TURNED, kv_heads), h)
        return pair, h

    def slots_of(pair, h):
        forward = h < TURNED
        one = jnp.where(forward | (pair == 0), 2 * pair + 1 - core, 2 * pair + 1)
        two = jnp.where(
            forward,
            2 * pair + 2 - core,
            jnp.where((pair == 0) & (core == 1), 1, 2 * (REACH - pair)),
        )
        return one, two

    def missing(slot):
        return ((slot - 1 + core) * rows).astype(jnp.float32) - before

    def prepare(slots):
        for part, slot in enumerate(slots):
            own = slot == own_slot
            angle = -missing(slot) * freq_row
            c, s = jnp.cos(angle), jnp.sin(angle)

            @pl.when(own)
            def _():
                blk_cos[part] = own_cos[...]
                blk_sin[part] = own_sin[...]

            @pl.when(jnp.logical_not(own))
            def _():
                blk_cos[part] = tables[0] * c - tables[1] * s
                blk_sin[part] = (tables[1] * c + tables[0] * s) * sign

    def load_keys(q):
        pair, h = split(q)
        for part, slot in enumerate(slots_of(pair, h)):
            turned = rotate(kv[slot, h, 0], blk_cos[part], blk_sin[part])
            turned = jnp.where(sublane < missing(slot), anchor[h][:1], turned)
            kx[part * rows : (part + 1) * rows] = turned.astype(jnp.bfloat16)

    def load_values(q):
        pair, h = split(q)
        at = lax.broadcasted_iota(jnp.int32, (vt.shape[0] - HD, rows), 1).astype(jnp.float32)
        for part, slot in enumerate(slots_of(pair, h)):
            span = slice(part * rows, (part + 1) * rows)
            kept = jnp.where(sublane < missing(slot), 0.0, kv[slot, h, 1].astype(jnp.float32))
            vt[:HD, span] = kept.astype(jnp.bfloat16).T
            vt[HD:, span] = jnp.where(at < missing(slot), 0.0, 1.0).astype(jnp.bfloat16)

    def receive(q):
        pair, h = split(q)
        forward = h < TURNED
        back = h >= TURNED
        far = REACH - pair

        ahead = 2 * pair + 3 - core
        mine = (pair < REACH - 1) & (chip >= pair + 1) & ((core == 0) | forward)

        @pl.when(mine)
        def _():
            hop(ahead - 2, h).wait_recv()
            side(ahead, h).start()

        @pl.when(mine & (chip < last) & (pair < REACH - 2))
        def _():
            hop(ahead, h).start()

        @pl.when(mine & (chip < last) & (pair == REACH - 2) & (core == 1))
        def _():
            last_hop(ahead, h).start()

        @pl.when(back & (pair == 0) & (core == 1) & (relayed < last))
        def _():
            first_leg(h).wait_recv()
            second_leg(h).start()

        chained = back & (core == 0) & (chip >= far)

        @pl.when(chained)
        def _():
            side(2 * far, h).wait_recv()

        @pl.when(chained & (far >= 2))
        def _():
            back_hop(2 * far, h).start()

        @pl.when(chained & (far < REACH))
        def _():
            side(2 * far, h).start()

        one, two = slots_of(pair, h)

        @pl.when((h == 0) | (h == TURNED))
        def _():
            prepare((one, two))

        @pl.when(back & (pair > 0) & (core == 1) & (chip >= pair))
        def _():
            side(one, h).wait_recv()

        @pl.when((chip >= two // 2) & (forward | (core == 1)))
        def _():
            side(two, h).wait_recv()

    def score(q, u, own):
        _, h = split(q)
        t = h * group + u
        peak = None
        for at in range(0, 2 * rows, STRIP):
            scores = jnp.dot(kx[at : at + STRIP], qt[t], preferred_element_type=jnp.float32)
            if own:
                scores += diag[at : at + STRIP] if at < rows else allowed_row
            raw[u, at : at + STRIP] = scores
            top_here = jnp.max(scores.reshape(STRIP // 8, 8, rows), axis=0)
            peak = top_here if peak is None else jnp.maximum(peak, top_here)
        peaks[u] = peak if own else jnp.where(first_row, peak, -BIG)

    def weigh(q, u):
        pair, h = split(q)
        t = h * group + u
        old = top[t]
        peak = jnp.maximum(old, jnp.max(peaks[u], axis=0, keepdims=True))
        fade = jnp.exp2((old - peak) * SCALE)
        shift = jnp.where(first_row | (pair == 0), peak * SCALE, BIG)
        shift = jnp.broadcast_to(shift, (8, rows))
        top[t] = peak
        weights = []
        for at in range(0, 2 * rows, STRIP):
            scores = raw[u, at : at + STRIP].reshape(STRIP // 8, 8, rows)
            part = jnp.exp2(scores * SCALE - shift[None])
            weights.append(part.reshape(STRIP, rows).astype(jnp.bfloat16))
        acc[t] = acc[t] * fade + jnp.dot(
            vt[...], jnp.concatenate(weights, axis=0), preferred_element_type=jnp.float32
        )

    def store(h):
        at = pl.multiple_of(h * group * HD, group * HD)
        return pltpu.make_async_copy(
            ovm.at[h], out.at[:, pl.ds(at, group * HD)], out_sem.at[h]
        )

    def finish(q):
        _, h = split(q)
        for g in range(group):
            t = h * group + g
            share = 1.0 / acc[t, HD : HD + 1]
            ovm[h, :, g * HD : (g + 1) * HD] = (acc[t, :HD] * share).astype(jnp.bfloat16).T
        store(h).start()

    def step(q, own):
        receive(q)
        load_keys(q)
        load_values(q - 1)
        for u in range(group):
            weigh(q - 1, u)
            score(q, u, own)

    first = jnp.int32(0)
    receive(first)
    load_keys(first)
    for u in range(group):
        score(first, u, True)

    def own_step(q, carry):
        step(q, True)
        return carry

    lax.fori_loop(1, kv_heads, own_step, 0)

    def later_step(q, carry):
        @pl.when(q >= chunks - kv_heads + 2)
        def _():
            finish(q - 2)

        step(q, False)
        return carry

    lax.fori_loop(kv_heads, chunks, later_step, 0)
    final = jnp.int32(chunks - 1)
    load_values(final)
    finish(final - 1)
    for u in range(group):
        weigh(final, u)
    finish(final)

    def drain(copy, when):
        @pl.when(when)
        def _():
            copy.wait_send()

    for o in range(1, SPAN + 1):
        drain(seg_copy(o), me + o < n)
    for h in range(kv_heads):
        lane_here = (core == 0) | (h < TURNED)
        for j in range(REACH):
            slot = 2 * j + own_slot
            sends = lane_here & (chip >= j) & (chip < last)
            if j == REACH - 1:
                sends = sends & (core == 1)
            drain(hop(slot, h), sends)
            drain(side(slot, h), (lane_here & (chip >= j)) if j else core == 0)
        if h >= TURNED:
            drain(first_leg(h), (core == 1) & (chip < last))
            drain(second_leg(h), (core == 1) & (relayed < last))
            for j in range(1, REACH + 1):
                turned = (core == 0) & (chip >= j)
                if j >= 2:
                    drain(back_hop(2 * j, h), turned)
                if j < REACH:
                    drain(side(2 * j, h), turned)
        store(h).wait()
    rk_store.wait()


def local(queries, keys, values, segment_ids):
    rows, width = queries.shape
    kv_width = keys.shape[1]
    heads, kv_heads = width // HD, kv_width // HD
    group = heads // kv_heads
    half = HD // 2
    freq = (ROPE_BASE ** (-(np.arange(half) * (2.0 / HD)))).astype(np.float32)
    freq = np.concatenate([freq, freq])[None]
    angle = (np.arange(rows, dtype=np.float32)[:, None] * freq).astype(np.float64)
    table = np.stack([np.cos(angle), np.sin(angle)]).astype(np.float32)
    any_space = pl.BlockSpec(memory_space=pl.ANY)
    bf16, f32 = jnp.bfloat16, jnp.float32
    slots = 2 * REACH + 1
    dma = pltpu.SemaphoreType.DMA
    return pl.pallas_call(
        functools.partial(kernel, kv_heads, group),
        out_shape=(
            jax.ShapeDtypeStruct((rows, width), bf16),
            jax.ShapeDtypeStruct((rows, kv_width), bf16),
        ),
        in_specs=[any_space] * 6,
        out_specs=(any_space, any_space),
        scratch_shapes=[
            pltpu.VMEM((SPAN + 1, 1, rows), jnp.int32),
            pltpu.VMEM((rows, width), bf16),
            pltpu.VMEM((slots, kv_heads, 2, rows, HD), bf16),
            pltpu.VMEM((2, rows, HD), f32),
            pltpu.VMEM((1, HD), f32),
            pltpu.VMEM((heads, HD, rows), bf16),
            pltpu.VMEM((rows, rows), f32),
            pltpu.VMEM((rows, HD), f32),
            pltpu.VMEM((rows, HD), f32),
            pltpu.VMEM((2, rows, HD), f32),
            pltpu.VMEM((2, rows, HD), f32),
            pltpu.VMEM((2 * rows, HD), bf16),
            pltpu.VMEM((HD + 16, 2 * rows), bf16),
            pltpu.VMEM((heads, 1, rows), f32),
            pltpu.VMEM((kv_heads, 8, HD), f32),
            pltpu.VMEM((heads, HD + 16, rows), f32),
            pltpu.VMEM((group, 2 * rows, rows), f32),
            pltpu.VMEM((group, 8, rows), f32),
            pltpu.VMEM((kv_heads, rows, group * HD), bf16),
            pltpu.VMEM((rows, kv_width), bf16),
            dma((4 + 2 * kv_heads,)),
            dma((SPAN,)),
            dma((SPAN,)),
            dma((slots, kv_heads)),
            dma((slots, kv_heads)),
            dma((slots, kv_heads)),
            pltpu.VMEM((kv_heads - TURNED, 2, rows, HD), bf16),
            dma((kv_heads - TURNED,)),
            dma((kv_heads - TURNED,)),
            dma((kv_heads - TURNED,)),
            dma((slots, kv_heads)),
            dma((kv_heads,)),
        ],
        compiler_params=pltpu.CompilerParams(
            collective_id=0, has_side_effects=True, vmem_limit_bytes=56 * 1024 * 1024
        ),
    )(
        segment_ids.reshape(1, rows),
        queries,
        keys,
        values,
        jnp.asarray(table),
        jnp.asarray(freq),
    )


def solution(mesh):
    both = ("groups", "seq")
    return jax.shard_map(
        local,
        mesh=mesh,
        in_specs=(P(both, None), P(both, None), P(both, None), P(both)),
        out_specs=(P(both, None), P(both, None)),
        check_vma=False,
    )
```

```python
import functools
import math

import jax
import jax.numpy as jnp
import numpy as np
from jax import lax
from jax.experimental import pallas as pl
from jax.experimental.pallas import tpu as pltpu
from jax.sharding import PartitionSpec as P

HD = 128
SPAN = 7
REACH = 4
STRIP = 128
TURNED = 2
ROPE_BASE = 1000000.0
SCALE = float(HD ** (-0.5) * np.log2(np.e))
BIG = float(2.0**100)


def rotate(x, cosine, signed_sine):
    x = x.astype(jnp.float32)
    return x * cosine + pltpu.roll(x, HD // 2, 1) * signed_sine


def kernel(
    kv_heads,
    group,
    seg_in,
    q_in,
    k_in,
    v_in,
    table_in,
    freq_in,
    out,
    rk_out,
    segs,
    qraw,
    kv,
    tables,
    freq,
    qt,
    diag,
    own_cos,
    own_sin,
    blk_cos,
    blk_sin,
    kx,
    vt,
    top,
    anchor,
    acc,
    raw,
    peaks,
    ovm,
    rkvm,
    in_sem,
    seg_send,
    seg_recv,
    hop_send,
    side_send,
    chain_send,
    via,
    via_send,
    via_recv,
    leg_send,
    kv_recv,
    out_sem,
):
    rows = q_in.shape[0]
    half = HD // 2
    me = lax.axis_index("seq")
    n = lax.axis_size("seq")
    core = lax.rem(me, 2)
    own_slot = 1 - core
    chip = me // 2
    last = n // 2 - 1
    width = math.isqrt(n // 2)

    def device(offset):
        return {"seq": me + offset}

    def relay_of(source):
        return source // width * width + lax.rem(source + width - 2, width)

    def far_of(source):
        return jnp.minimum(source + REACH, last)

    relayed = chip // width * width + lax.rem(chip + 2, width)

    seg_load = pltpu.make_async_copy(seg_in, segs.at[0], in_sem.at[0])
    seg_load.start()
    kv_loads = []
    for h in range(kv_heads):
        cols = slice(h * HD, (h + 1) * HD)
        for w, src in ((0, k_in), (1, v_in)):
            load = pltpu.make_async_copy(
                src.at[:, cols], kv.at[own_slot, h, w], in_sem.at[4 + 2 * h + w]
            )
            load.start()
            kv_loads.append(load)
    freq_load = pltpu.make_async_copy(freq_in, freq, in_sem.at[1])
    freq_load.start()
    table_load = pltpu.make_async_copy(table_in, tables, in_sem.at[2])
    table_load.start()
    q_load = pltpu.make_async_copy(q_in, qraw, in_sem.at[3])
    q_load.start()

    barrier = pltpu.get_barrier_semaphore()

    def tell(rank, when):
        @pl.when(when)
        def _():
            pl.semaphore_signal(barrier, 1, device_id={"seq": rank})

    for o in range(1, SPAN + 1):
        tell(me - o, me >= o)
    tell(me + 1, (core == 0) & (chip >= 1))
    tell(me + 2, (core == 0) & (chip >= 1) & (chip < last))
    tell(2 * relayed + 1, (core == 1) & (relayed < last))
    tell(2 * relay_of(chip - REACH) + 1, (core == 0) & (chip >= REACH))
    for back in range(1, REACH):
        tell(2 * relay_of(chip - back) + 1, (core == 0) & (chip == last))
    receivers = jnp.minimum(SPAN, n - 1 - me) + jnp.where(
        core == 0,
        jnp.where(chip >= 2, 1, 0),
        jnp.where(chip >= 1, 1, 0)
        + jnp.where(chip < last, 1, 0)
        + jnp.where(relayed < last, 1, 0),
    )
    pl.semaphore_wait(barrier, receivers)

    seg_load.wait()
    def seg_copy(o):
        return pltpu.make_async_remote_copy(
            src_ref=segs.at[0],
            dst_ref=segs.at[o],
            send_sem=seg_send.at[o - 1],
            recv_sem=seg_recv.at[o - 1],
            device_id=device(o),
        )

    for o in range(1, SPAN + 1):

        @pl.when(me + o < n)
        def _():
            seg_copy(o).start()

    def hop(slot, h):
        return pltpu.make_async_remote_copy(
            src_ref=kv.at[slot, h],
            dst_ref=kv.at[slot + 2, h],
            send_sem=hop_send.at[slot, h],
            recv_sem=kv_recv.at[slot + 2, h],
            device_id=device(2),
        )

    def last_hop(slot, h):
        return pltpu.make_async_remote_copy(
            src_ref=kv.at[slot, h],
            dst_ref=kv.at[slot + 2, h],
            send_sem=hop_send.at[slot, h],
            recv_sem=kv_recv.at[slot + 2, h],
            device_id=device(1),
        )

    def side(slot, h):
        return pltpu.make_async_remote_copy(
            src_ref=kv.at[slot, h],
            dst_ref=kv.at[slot, h],
            send_sem=side_send.at[slot, h],
            recv_sem=kv_recv.at[slot, h],
            device_id=device(1 - 2 * core),
        )

    def back_hop(slot, h):
        return pltpu.make_async_remote_copy(
            src_ref=kv.at[slot, h],
            dst_ref=kv.at[slot - 2, h],
            send_sem=chain_send.at[slot, h],
            recv_sem=kv_recv.at[slot - 2, h],
            device_id=device(-2),
        )

    def first_leg(h):
        return pltpu.make_async_remote_copy(
            src_ref=kv.at[own_slot, h],
            dst_ref=via.at[h - TURNED],
            send_sem=via_send.at[h - TURNED],
            recv_sem=via_recv.at[h - TURNED],
            device_id={"seq": 2 * relay_of(chip) + 1},
        )

    def second_leg(h):
        far = far_of(relayed)
        slot = 2 * (far - relayed)
        return pltpu.make_async_remote_copy(
            src_ref=via.at[h - TURNED],
            dst_ref=kv.at[slot, h],
            send_sem=leg_send.at[h - TURNED],
            recv_sem=kv_recv.at[slot, h],
            device_id={"seq": 2 * far},
        )

    for h in range(kv_heads):
        kv_loads[2 * h].wait()
        kv_loads[2 * h + 1].wait()

        @pl.when((chip < last) & ((core == 0) | (h < TURNED)))
        def _():
            hop(own_slot, h).start()

        if h >= TURNED:

            @pl.when((chip < last) & (core == 1))
            def _():
                first_leg(h).start()

        @pl.when(core == 0)
        def _():
            side(own_slot, h).start()

    def blank(slot, carry):
        @pl.when(chip < slot // 2)
        def _():
            kv[slot] = jnp.zeros(kv.shape[1:], kv.dtype)

        return carry

    lax.fori_loop(2, 2 * REACH + 1, blank, 0)

    def relay(j, h, early):
        ahead = 2 * j + 1 - core
        before_ids = (chip < REACH) & (j < chip)
        mine = (j < REACH) & (chip >= j) & ((core == 0) | (h < TURNED))
        mine = mine & (before_ids if early else jnp.logical_not(before_ids))

        @pl.when(mine)
        def _():
            hop(ahead - 2, h).wait_recv()
            side(ahead, h).start()

        @pl.when(mine & (chip < last) & (j < REACH - 1))
        def _():
            hop(ahead, h).start()

        @pl.when(mine & (chip < last) & (j == REACH - 1) & (core == 1))
        def _():
            last_hop(ahead, h).start()

    def turn_back(early):
        when = (core == 1) & (relayed < last)
        when = when & ((chip < REACH) if early else (chip >= REACH))

        @pl.when(when)
        def _():
            for h in range(TURNED, kv_heads):
                first_leg(h).wait_recv()
                second_leg(h).start()

    freq_load.wait()
    table_load.wait()
    lane = lax.broadcasted_iota(jnp.int32, (rows, HD), 1)
    sublane = lax.broadcasted_iota(jnp.int32, (rows, HD), 0).astype(jnp.float32)
    sign = jnp.where(lane < half, -1.0, 1.0)
    freq_row = freq[...]
    seg_row = segs[0]
    seg_first = seg_row[:, :1]
    first_row = seg_row == seg_first
    seg_wide = jnp.broadcast_to(seg_row.astype(jnp.float32), (rows, rows))
    seg_tall = seg_wide.T
    key_at = lax.broadcasted_iota(jnp.int32, (rows, rows), 0)
    row_at = lax.broadcasted_iota(jnp.int32, (rows, rows), 1)
    same = seg_tall == seg_wide
    diag[...] = jnp.where(same & (key_at <= row_at), 0.0, -BIG)
    local_position = jnp.sum(
        jnp.where(same & (row_at < key_at), 1.0, 0.0), axis=1, keepdims=True
    )
    first_tall = seg_tall[:, :HD] == seg_first.astype(jnp.float32)
    local_angle = local_position * freq_row
    local_cos = jnp.cos(local_angle)
    local_sin = jnp.sin(local_angle)
    def clear(t, carry):
        top[t] = jnp.full((1, rows), -4.0 * BIG, jnp.float32)
        acc[t] = jnp.zeros(acc.shape[1:], jnp.float32)
        return carry

    lax.fori_loop(0, kv_heads * group, clear, 0)

    turn_back(True)

    def early_relay(i, carry):
        relay(i // kv_heads, lax.rem(i, kv_heads), True)
        return carry

    lax.fori_loop(kv_heads, (REACH - 1) * kv_heads, early_relay, 0)

    for o in range(1, SPAN + 1):

        @pl.when(me >= o)
        def _():
            seg_copy(o).wait_recv()

        @pl.when(me < o)
        def _():
            segs[o] = jnp.full((1, rows), -1, jnp.int32)

    hits = jnp.zeros_like(seg_row, jnp.float32)
    for o in range(1, SPAN + 1):
        hits += jnp.where(segs[o] == seg_first, 1.0, 0.0)
    before = jnp.sum(hits, axis=1, keepdims=True)
    base_angle = before * freq_row
    base_cos = jnp.where(first_tall, jnp.cos(base_angle), 1.0)
    base_sin = jnp.where(first_tall, jnp.sin(base_angle), 0.0)
    own_cos[...] = local_cos * base_cos - local_sin * base_sin
    own_sin[...] = (local_sin * base_cos + local_cos * base_sin) * sign

    for h in range(kv_heads):
        turned_keys = rotate(kv[own_slot, h, 0], own_cos[...], own_sin[...])
        anchor[h] = turned_keys[:8]
        rkvm[:, h * HD : (h + 1) * HD] = turned_keys.astype(jnp.bfloat16)
    rk_store = pltpu.make_async_copy(rkvm, rk_out, in_sem.at[0])
    rk_store.start()

    q_load.wait()

    def turn(t, carry):
        at = pl.multiple_of(t * HD, HD)
        turned = rotate(qraw[:, pl.ds(at, HD)], own_cos[...], own_sin[...])
        qt[t] = turned.astype(jnp.bfloat16).T
        return carry

    lax.fori_loop(0, kv_heads * group, turn, 0)
    turn_back(False)

    chunks = (SPAN + 1) // 2 * kv_heads
    allowed_row = jnp.where(first_row, 0.0, -BIG)

    def split(q):
        part, i = q // kv_heads, lax.rem(q, kv_heads)
        pair = jnp.where(part < 2, i // TURNED, part)
        h = jnp.where(
            part < 2,
            lax.rem(i, TURNED) + TURNED * part,
            jnp.where(part == REACH - 1, lax.rem(i + TURNED, kv_heads), i),
        )
        return pair, h

    def slots_of(pair, h):
        forward = h < TURNED
        one = jnp.where(forward | (pair == 0), 2 * pair + 1 - core, 2 * pair + 1)
        two = jnp.where(
            forward,
            2 * pair + 2 - core,
            jnp.where((pair == 0) & (core == 1), 1, 2 * (REACH - pair)),
        )
        return one, two

    def missing(slot):
        return ((slot - 1 + core) * rows).astype(jnp.float32) - before

    def prepare(slots):
        for part, slot in enumerate(slots):
            own = slot == own_slot
            angle = -missing(slot) * freq_row
            c, s = jnp.cos(angle), jnp.sin(angle)

            @pl.when(own)
            def _():
                blk_cos[part] = own_cos[...]
                blk_sin[part] = own_sin[...]

            @pl.when(jnp.logical_not(own))
            def _():
                blk_cos[part] = tables[0] * c - tables[1] * s
                blk_sin[part] = (tables[1] * c + tables[0] * s) * sign

    def load_keys(q):
        pair, h = split(q)
        for part, slot in enumerate(slots_of(pair, h)):
            turned = rotate(kv[slot, h, 0], blk_cos[part], blk_sin[part])
            turned = jnp.where(sublane < missing(slot), anchor[h][:1], turned)
            kx[part * rows : (part + 1) * rows] = turned.astype(jnp.bfloat16)

    def load_values(q):
        pair, h = split(q)
        at = lax.broadcasted_iota(jnp.int32, (vt.shape[0] - HD, rows), 1).astype(jnp.float32)
        for part, slot in enumerate(slots_of(pair, h)):
            span = slice(part * rows, (part + 1) * rows)
            kept = jnp.where(sublane < missing(slot), 0.0, kv[slot, h, 1].astype(jnp.float32))
            vt[:HD, span] = kept.astype(jnp.bfloat16).T
            vt[HD:, span] = jnp.where(at < missing(slot), 0.0, 1.0).astype(jnp.bfloat16)

    def receive(q):
        pair, h = split(q)
        forward = h < TURNED
        back = h >= TURNED
        far = REACH - pair

        @pl.when(forward & (pair == 1))
        def _():
            @pl.when(h == 0)
            def _():
                for g in range(TURNED, kv_heads):
                    relay(1, g, False)

        turn_ahead = jnp.where(forward | (pair >= 2), pair + 1, 2)

        @pl.when(forward | (pair != 1))
        def _():
            relay(turn_ahead, h, False)

        chained = back & (core == 0) & (chip >= far)

        @pl.when(chained)
        def _():
            side(2 * far, h).wait_recv()

        @pl.when(chained & (far >= 2))
        def _():
            back_hop(2 * far, h).start()

        @pl.when(chained & (far < REACH))
        def _():
            side(2 * far, h).start()

        one, two = slots_of(pair, h)

        @pl.when((h == 0) | (h == TURNED))
        def _():
            prepare((one, two))

        @pl.when(back & (pair > 0) & (core == 1) & (chip >= pair))
        def _():
            side(one, h).wait_recv()

        @pl.when((chip >= two // 2) & (forward | (core == 1)))
        def _():
            side(two, h).wait_recv()

    def score(q, u, own):
        _, h = split(q)
        t = h * group + u
        peak = None
        for at in range(0, 2 * rows, STRIP):
            scores = jnp.dot(kx[at : at + STRIP], qt[t], preferred_element_type=jnp.float32)
            if own:
                scores += diag[at : at + STRIP] if at < rows else allowed_row
            raw[u, at : at + STRIP] = scores
            top_here = jnp.max(scores.reshape(STRIP // 8, 8, rows), axis=0)
            peak = top_here if peak is None else jnp.maximum(peak, top_here)
        peaks[u] = peak if own else jnp.where(first_row, peak, -BIG)

    def weigh(q, u):
        pair, h = split(q)
        t = h * group + u
        old = top[t]
        peak = jnp.maximum(old, jnp.max(peaks[u], axis=0, keepdims=True))
        fade = jnp.exp2((old - peak) * SCALE)
        shift = jnp.where(first_row | (pair == 0), peak * SCALE, BIG)
        shift = jnp.broadcast_to(shift, (8, rows))
        top[t] = peak
        weights = []
        for at in range(0, 2 * rows, STRIP):
            scores = raw[u, at : at + STRIP].reshape(STRIP // 8, 8, rows)
            part = jnp.exp2(scores * SCALE - shift[None])
            weights.append(part.reshape(STRIP, rows).astype(jnp.bfloat16))
        acc[t] = acc[t] * fade + jnp.dot(
            vt[...], jnp.concatenate(weights, axis=0), preferred_element_type=jnp.float32
        )

    def store(h):
        at = pl.multiple_of(h * group * HD, group * HD)
        return pltpu.make_async_copy(
            ovm.at[h], out.at[:, pl.ds(at, group * HD)], out_sem.at[h]
        )

    def finish(q):
        _, h = split(q)
        for g in range(group):
            t = h * group + g
            share = 1.0 / acc[t, HD : HD + 1]
            ovm[h, :, g * HD : (g + 1) * HD] = (acc[t, :HD] * share).astype(jnp.bfloat16).T
        store(h).start()

    def step(q, own):
        receive(q)
        load_keys(q)
        load_values(q - 1)
        for u in range(group):
            weigh(q - 1, u)
            score(q, u, own)

    first = jnp.int32(0)
    receive(first)
    load_keys(first)
    for u in range(group):
        score(first, u, True)

    def every_step(q, carry):
        @pl.when(q >= chunks - kv_heads + 2)
        def _():
            finish(q - 2)

        pair, _ = split(q)

        @pl.when(pair == 0)
        def _():
            step(q, True)

        @pl.when(pair > 0)
        def _():
            step(q, False)

        return carry

    lax.fori_loop(1, chunks, every_step, 0)
    final = jnp.int32(chunks - 1)
    load_values(final)
    finish(final - 1)
    for u in range(group):
        weigh(final, u)
    finish(final)

    def drain(copy, when):
        @pl.when(when)
        def _():
            copy.wait_send()

    for o in range(1, SPAN + 1):
        drain(seg_copy(o), me + o < n)
    for h in range(kv_heads):
        lane_here = (core == 0) | (h < TURNED)
        for j in range(REACH):
            slot = 2 * j + own_slot
            sends = lane_here & (chip >= j) & (chip < last)
            if j == REACH - 1:
                sends = sends & (core == 1)
            drain(hop(slot, h), sends)
            drain(side(slot, h), (lane_here & (chip >= j)) if j else core == 0)
        if h >= TURNED:
            drain(first_leg(h), (core == 1) & (chip < last))
            drain(second_leg(h), (core == 1) & (relayed < last))
            for j in range(1, REACH + 1):
                turned = (core == 0) & (chip >= j)
                if j >= 2:
                    drain(back_hop(2 * j, h), turned)
                if j < REACH:
                    drain(side(2 * j, h), turned)
        store(h).wait()
    rk_store.wait()


def local(queries, keys, values, segment_ids):
    rows, width = queries.shape
    kv_width = keys.shape[1]
    heads, kv_heads = width // HD, kv_width // HD
    group = heads // kv_heads
    half = HD // 2
    freq = (ROPE_BASE ** (-(np.arange(half) * (2.0 / HD)))).astype(np.float32)
    freq = np.concatenate([freq, freq])[None]
    angle = (np.arange(rows, dtype=np.float32)[:, None] * freq).astype(np.float64)
    table = np.stack([np.cos(angle), np.sin(angle)]).astype(np.float32)
    any_space = pl.BlockSpec(memory_space=pl.ANY)
    bf16, f32 = jnp.bfloat16, jnp.float32
    slots = 2 * REACH + 1
    dma = pltpu.SemaphoreType.DMA
    return pl.pallas_call(
        functools.partial(kernel, kv_heads, group),
        out_shape=(
            jax.ShapeDtypeStruct((rows, width), bf16),
            jax.ShapeDtypeStruct((rows, kv_width), bf16),
        ),
        in_specs=[any_space] * 6,
        out_specs=(any_space, any_space),
        scratch_shapes=[
            pltpu.VMEM((SPAN + 1, 1, rows), jnp.int32),
            pltpu.VMEM((rows, width), bf16),
            pltpu.VMEM((slots, kv_heads, 2, rows, HD), bf16),
            pltpu.VMEM((2, rows, HD), f32),
            pltpu.VMEM((1, HD), f32),
            pltpu.VMEM((heads, HD, rows), bf16),
            pltpu.VMEM((rows, rows), f32),
            pltpu.VMEM((rows, HD), f32),
            pltpu.VMEM((rows, HD), f32),
            pltpu.VMEM((2, rows, HD), f32),
            pltpu.VMEM((2, rows, HD), f32),
            pltpu.VMEM((2 * rows, HD), bf16),
            pltpu.VMEM((HD + 16, 2 * rows), bf16),
            pltpu.VMEM((heads, 1, rows), f32),
            pltpu.VMEM((kv_heads, 8, HD), f32),
            pltpu.VMEM((heads, HD + 16, rows), f32),
            pltpu.VMEM((group, 2 * rows, rows), f32),
            pltpu.VMEM((group, 8, rows), f32),
            pltpu.VMEM((kv_heads, rows, group * HD), bf16),
            pltpu.VMEM((rows, kv_width), bf16),
            dma((4 + 2 * kv_heads,)),
            dma((SPAN,)),
            dma((SPAN,)),
            dma((slots, kv_heads)),
            dma((slots, kv_heads)),
            dma((slots, kv_heads)),
            pltpu.VMEM((kv_heads - TURNED, 2, rows, HD), bf16),
            dma((kv_heads - TURNED,)),
            dma((kv_heads - TURNED,)),
            dma((kv_heads - TURNED,)),
            dma((slots, kv_heads)),
            dma((kv_heads,)),
        ],
        compiler_params=pltpu.CompilerParams(
            collective_id=0, has_side_effects=True, vmem_limit_bytes=56 * 1024 * 1024
        ),
    )(
        segment_ids.reshape(1, rows),
        queries,
        keys,
        values,
        jnp.asarray(table),
        jnp.asarray(freq),
    )


def solution(mesh):
    both = ("groups", "seq")
    return jax.shard_map(
        local,
        mesh=mesh,
        in_specs=(P(both, None), P(both, None), P(both, None), P(both)),
        out_specs=(P(both, None), P(both, None)),
        check_vma=False,
    )
```

```python
import functools
import math

import jax
import jax.numpy as jnp
import numpy as np
from jax import lax
from jax.experimental import pallas as pl
from jax.experimental.pallas import tpu as pltpu
from jax.sharding import PartitionSpec as P

HD = 128
SPAN = 7
REACH = 4
STRIP = 128
TURNED = 2
ROPE_BASE = 1000000.0
SCALE = float(HD ** (-0.5) * np.log2(np.e))
BIG = float(2.0**100)


def rotate(x, cosine, signed_sine):
    x = x.astype(jnp.float32)
    return x * cosine + pltpu.roll(x, HD // 2, 1) * signed_sine


def kernel(
    kv_heads,
    group,
    seg_in,
    q_in,
    k_in,
    v_in,
    table_in,
    freq_in,
    out,
    rk_out,
    segs,
    qraw,
    kv,
    tables,
    freq,
    qt,
    diag,
    own_cos,
    own_sin,
    blk_cos,
    blk_sin,
    kx,
    vt,
    top,
    anchor,
    acc,
    raw,
    peaks,
    in_sem,
    seg_send,
    seg_recv,
    hop_send,
    side_send,
    chain_send,
    via,
    via_send,
    via_recv,
    leg_send,
    kv_recv,
):
    rows = q_in.shape[0]
    half = HD // 2
    me = lax.axis_index("seq")
    n = lax.axis_size("seq")
    core = lax.rem(me, 2)
    own_slot = 1 - core
    chip = me // 2
    last = n // 2 - 1
    width = math.isqrt(n // 2)

    def device(offset):
        return {"seq": me + offset}

    def relay_of(source):
        return source // width * width + lax.rem(source + width - 2, width)

    def far_of(source):
        return jnp.minimum(source + REACH, last)

    relayed = chip // width * width + lax.rem(chip + 2, width)

    seg_load = pltpu.make_async_copy(seg_in, segs.at[0], in_sem.at[0])
    seg_load.start()
    kv_loads = []
    for h in range(kv_heads):
        cols = slice(h * HD, (h + 1) * HD)
        for w, src in ((0, k_in), (1, v_in)):
            load = pltpu.make_async_copy(
                src.at[:, cols], kv.at[own_slot, h, w], in_sem.at[4 + 2 * h + w]
            )
            load.start()
            kv_loads.append(load)
    freq_load = pltpu.make_async_copy(freq_in, freq, in_sem.at[1])
    freq_load.start()
    table_load = pltpu.make_async_copy(table_in, tables, in_sem.at[2])
    table_load.start()
    q_load = pltpu.make_async_copy(q_in, qraw, in_sem.at[3])
    q_load.start()

    barrier = pltpu.get_barrier_semaphore()

    def tell(rank, when):
        @pl.when(when)
        def _():
            pl.semaphore_signal(barrier, 1, device_id={"seq": rank})

    for o in range(1, SPAN + 1):
        tell(me - o, me >= o)
    tell(me + 1, (core == 0) & (chip >= 1))
    tell(me + 2, (core == 0) & (chip >= 1) & (chip < last))
    tell(2 * relayed + 1, (core == 1) & (relayed < last))
    tell(2 * relay_of(chip - REACH) + 1, (core == 0) & (chip >= REACH))
    for back in range(1, REACH):
        tell(2 * relay_of(chip - back) + 1, (core == 0) & (chip == last))
    receivers = jnp.minimum(SPAN, n - 1 - me) + jnp.where(
        core == 0,
        jnp.where(chip >= 2, 1, 0),
        jnp.where(chip >= 1, 1, 0)
        + jnp.where(chip < last, 1, 0)
        + jnp.where(relayed < last, 1, 0),
    )
    pl.semaphore_wait(barrier, receivers)

    seg_load.wait()
    def seg_copy(o):
        return pltpu.make_async_remote_copy(
            src_ref=segs.at[0],
            dst_ref=segs.at[o],
            send_sem=seg_send.at[o - 1],
            recv_sem=seg_recv.at[o - 1],
            device_id=device(o),
        )

    for o in range(1, SPAN + 1):

        @pl.when(me + o < n)
        def _():
            seg_copy(o).start()

    def hop(slot, h):
        return pltpu.make_async_remote_copy(
            src_ref=kv.at[slot, h],
            dst_ref=kv.at[slot + 2, h],
            send_sem=hop_send.at[slot, h],
            recv_sem=kv_recv.at[slot + 2, h],
            device_id=device(2),
        )

    def last_hop(slot, h):
        return pltpu.make_async_remote_copy(
            src_ref=kv.at[slot, h],
            dst_ref=kv.at[slot + 2, h],
            send_sem=hop_send.at[slot, h],
            recv_sem=kv_recv.at[slot + 2, h],
            device_id=device(1),
        )

    def side(slot, h):
        return pltpu.make_async_remote_copy(
            src_ref=kv.at[slot, h],
            dst_ref=kv.at[slot, h],
            send_sem=side_send.at[slot, h],
            recv_sem=kv_recv.at[slot, h],
            device_id=device(1 - 2 * core),
        )

    def back_hop(slot, h):
        return pltpu.make_async_remote_copy(
            src_ref=kv.at[slot, h],
            dst_ref=kv.at[slot - 2, h],
            send_sem=chain_send.at[slot, h],
            recv_sem=kv_recv.at[slot - 2, h],
            device_id=device(-2),
        )

    def first_leg(h):
        return pltpu.make_async_remote_copy(
            src_ref=kv.at[own_slot, h],
            dst_ref=via.at[h - TURNED],
            send_sem=via_send.at[h - TURNED],
            recv_sem=via_recv.at[h - TURNED],
            device_id={"seq": 2 * relay_of(chip) + 1},
        )

    def second_leg(h):
        far = far_of(relayed)
        slot = 2 * (far - relayed)
        return pltpu.make_async_remote_copy(
            src_ref=via.at[h - TURNED],
            dst_ref=kv.at[slot, h],
            send_sem=leg_send.at[h - TURNED],
            recv_sem=kv_recv.at[slot, h],
            device_id={"seq": 2 * far},
        )

    for h in range(kv_heads):
        kv_loads[2 * h].wait()
        kv_loads[2 * h + 1].wait()

        @pl.when((chip < last) & ((core == 0) | (h < TURNED)))
        def _():
            hop(own_slot, h).start()

        if h >= TURNED:

            @pl.when((chip < last) & (core == 1))
            def _():
                first_leg(h).start()

        @pl.when(core == 0)
        def _():
            side(own_slot, h).start()

    def blank(slot, carry):
        @pl.when(chip < slot // 2)
        def _():
            kv[slot] = jnp.zeros(kv.shape[1:], kv.dtype)

        return carry

    lax.fori_loop(2, 2 * REACH + 1, blank, 0)

    def relay(j, h, early):
        ahead = 2 * j + 1 - core
        before_ids = (chip < REACH) & (j < chip)
        mine = (j < REACH) & (chip >= j) & ((core == 0) | (h < TURNED))
        mine = mine & (before_ids if early else jnp.logical_not(before_ids))

        @pl.when(mine)
        def _():
            hop(ahead - 2, h).wait_recv()
            side(ahead, h).start()

        @pl.when(mine & (chip < last) & (j < REACH - 1))
        def _():
            hop(ahead, h).start()

        @pl.when(mine & (chip < last) & (j == REACH - 1) & (core == 1))
        def _():
            last_hop(ahead, h).start()

    def turn_back(early):
        when = (core == 1) & (relayed < last)
        when = when & ((chip < REACH) if early else (chip >= REACH))

        @pl.when(when)
        def _():
            for h in range(TURNED, kv_heads):
                first_leg(h).wait_recv()
                second_leg(h).start()

    freq_load.wait()
    table_load.wait()
    lane = lax.broadcasted_iota(jnp.int32, (rows, HD), 1)
    sublane = lax.broadcasted_iota(jnp.int32, (rows, HD), 0).astype(jnp.float32)
    sign = jnp.where(lane < half, -1.0, 1.0)
    freq_row = freq[...]
    seg_row = segs[0]
    seg_first = seg_row[:, :1]
    first_row = seg_row == seg_first
    seg_wide = jnp.broadcast_to(seg_row.astype(jnp.float32), (rows, rows))
    seg_tall = seg_wide.T
    key_at = lax.broadcasted_iota(jnp.int32, (rows, rows), 0)
    row_at = lax.broadcasted_iota(jnp.int32, (rows, rows), 1)
    same = seg_tall == seg_wide
    diag[...] = jnp.where(same & (key_at <= row_at), 0.0, -BIG)
    local_position = jnp.sum(
        jnp.where(same & (row_at < key_at), 1.0, 0.0), axis=1, keepdims=True
    )
    first_tall = seg_tall[:, :HD] == seg_first.astype(jnp.float32)
    local_angle = local_position * freq_row
    local_cos = jnp.cos(local_angle)
    local_sin = jnp.sin(local_angle)
    def clear(t, carry):
        top[t] = jnp.full((1, rows), -4.0 * BIG, jnp.float32)
        acc[t] = jnp.zeros(acc.shape[1:], jnp.float32)
        return carry

    lax.fori_loop(0, kv_heads * group, clear, 0)

    turn_back(True)

    def early_relay(i, carry):
        relay(i // kv_heads, lax.rem(i, kv_heads), True)
        return carry

    lax.fori_loop(kv_heads, (REACH - 1) * kv_heads, early_relay, 0)

    for o in range(1, SPAN + 1):

        @pl.when(me >= o)
        def _():
            seg_copy(o).wait_recv()

        @pl.when(me < o)
        def _():
            segs[o] = jnp.full((1, rows), -1, jnp.int32)

    hits = jnp.zeros_like(seg_row, jnp.float32)
    for o in range(1, SPAN + 1):
        hits += jnp.where(segs[o] == seg_first, 1.0, 0.0)
    before = jnp.sum(hits, axis=1, keepdims=True)
    base_angle = before * freq_row
    base_cos = jnp.where(first_tall, jnp.cos(base_angle), 1.0)
    base_sin = jnp.where(first_tall, jnp.sin(base_angle), 0.0)
    own_cos[...] = local_cos * base_cos - local_sin * base_sin
    own_sin[...] = (local_sin * base_cos + local_cos * base_sin) * sign

    for h in range(kv_heads):
        turned_keys = rotate(kv[own_slot, h, 0], own_cos[...], own_sin[...])
        anchor[h] = turned_keys[:8]
        rk_out[:, h * HD : (h + 1) * HD] = turned_keys.astype(jnp.bfloat16)

    q_load.wait()

    def turn(t, carry):
        at = pl.multiple_of(t * HD, HD)
        turned = rotate(qraw[:, pl.ds(at, HD)], own_cos[...], own_sin[...])
        qt[t] = turned.astype(jnp.bfloat16).T
        return carry

    lax.fori_loop(0, kv_heads * group, turn, 0)
    turn_back(False)

    chunks = (SPAN + 1) // 2 * kv_heads
    allowed_row = jnp.where(first_row, 0.0, -BIG)

    def split(q):
        part, i = q // kv_heads, lax.rem(q, kv_heads)
        pair = jnp.where(part < 2, i // TURNED, part)
        h = jnp.where(
            part < 2,
            lax.rem(i, TURNED) + TURNED * part,
            jnp.where(part == REACH - 1, lax.rem(i + TURNED, kv_heads), i),
        )
        return pair, h

    def slots_of(pair, h):
        forward = h < TURNED
        one = jnp.where(forward | (pair == 0), 2 * pair + 1 - core, 2 * pair + 1)
        two = jnp.where(
            forward,
            2 * pair + 2 - core,
            jnp.where((pair == 0) & (core == 1), 1, 2 * (REACH - pair)),
        )
        return one, two

    def missing(slot):
        return ((slot - 1 + core) * rows).astype(jnp.float32) - before

    def prepare(slots):
        for part, slot in enumerate(slots):
            own = slot == own_slot
            angle = -missing(slot) * freq_row
            c, s = jnp.cos(angle), jnp.sin(angle)

            @pl.when(own)
            def _():
                blk_cos[part] = own_cos[...]
                blk_sin[part] = own_sin[...]

            @pl.when(jnp.logical_not(own))
            def _():
                blk_cos[part] = tables[0] * c - tables[1] * s
                blk_sin[part] = (tables[1] * c + tables[0] * s) * sign

    def load_keys(q):
        pair, h = split(q)
        for part, slot in enumerate(slots_of(pair, h)):
            turned = rotate(kv[slot, h, 0], blk_cos[part], blk_sin[part])
            turned = jnp.where(sublane < missing(slot), anchor[h][:1], turned)
            kx[part * rows : (part + 1) * rows] = turned.astype(jnp.bfloat16)

    def load_values(q):
        pair, h = split(q)
        at = lax.broadcasted_iota(jnp.int32, (vt.shape[0] - HD, rows), 1).astype(jnp.float32)
        for part, slot in enumerate(slots_of(pair, h)):
            span = slice(part * rows, (part + 1) * rows)
            kept = jnp.where(sublane < missing(slot), 0.0, kv[slot, h, 1].astype(jnp.float32))
            vt[:HD, span] = kept.astype(jnp.bfloat16).T
            vt[HD:, span] = jnp.where(at < missing(slot), 0.0, 1.0).astype(jnp.bfloat16)

    def receive(q):
        pair, h = split(q)
        forward = h < TURNED
        back = h >= TURNED
        far = REACH - pair

        @pl.when(forward & (pair == 1))
        def _():
            @pl.when(h == 0)
            def _():
                for g in range(TURNED, kv_heads):
                    relay(1, g, False)

        turn_ahead = jnp.where(forward | (pair >= 2), pair + 1, 2)

        @pl.when(forward | (pair != 1))
        def _():
            relay(turn_ahead, h, False)

        chained = back & (core == 0) & (chip >= far)

        @pl.when(chained)
        def _():
            side(2 * far, h).wait_recv()

        @pl.when(chained & (far >= 2))
        def _():
            back_hop(2 * far, h).start()

        @pl.when(chained & (far < REACH))
        def _():
            side(2 * far, h).start()

        one, two = slots_of(pair, h)

        @pl.when((h == 0) | (h == TURNED))
        def _():
            prepare((one, two))

        @pl.when(back & (pair > 0) & (core == 1) & (chip >= pair))
        def _():
            side(one, h).wait_recv()

        @pl.when((chip >= two // 2) & (forward | (core == 1)))
        def _():
            side(two, h).wait_recv()

    def score(q, u, own):
        _, h = split(q)
        t = h * group + u
        peak = None
        for at in range(0, 2 * rows, STRIP):
            scores = jnp.dot(kx[at : at + STRIP], qt[t], preferred_element_type=jnp.float32)
            if own:
                scores += diag[at : at + STRIP] if at < rows else allowed_row
            raw[u, at : at + STRIP] = scores
            top_here = jnp.max(scores.reshape(STRIP // 8, 8, rows), axis=0)
            peak = top_here if peak is None else jnp.maximum(peak, top_here)
        peaks[u] = peak if own else jnp.where(first_row, peak, -BIG)

    def weigh(q, u):
        pair, h = split(q)
        t = h * group + u
        old = top[t]
        peak = jnp.maximum(old, jnp.max(peaks[u], axis=0, keepdims=True))
        fade = jnp.exp2((old - peak) * SCALE)
        shift = jnp.where(first_row | (pair == 0), peak * SCALE, BIG)
        shift = jnp.broadcast_to(shift, (8, rows))
        top[t] = peak
        weights = []
        for at in range(0, 2 * rows, STRIP):
            scores = raw[u, at : at + STRIP].reshape(STRIP // 8, 8, rows)
            part = jnp.exp2(scores * SCALE - shift[None])
            weights.append(part.reshape(STRIP, rows).astype(jnp.bfloat16))
        acc[t] = acc[t] * fade + jnp.dot(
            vt[...], jnp.concatenate(weights, axis=0), preferred_element_type=jnp.float32
        )

    def finish(q):
        _, h = split(q)
        for g in range(group):
            t = h * group + g
            share = 1.0 / acc[t, HD : HD + 1]
            at = pl.multiple_of(t * HD, HD)
            out[:, pl.ds(at, HD)] = (acc[t, :HD] * share).astype(jnp.bfloat16).T

    def step(q, own):
        receive(q)
        load_keys(q)
        load_values(q - 1)
        for u in range(group):
            weigh(q - 1, u)
            score(q, u, own)

    first = jnp.int32(0)
    receive(first)
    load_keys(first)
    for u in range(group):
        score(first, u, True)

    def every_step(q, carry):
        @pl.when(q >= chunks - kv_heads + 2)
        def _():
            finish(q - 2)

        pair, _ = split(q)

        @pl.when(pair == 0)
        def _():
            step(q, True)

        @pl.when(pair > 0)
        def _():
            step(q, False)

        return carry

    lax.fori_loop(1, chunks, every_step, 0)
    final = jnp.int32(chunks - 1)
    load_values(final)
    finish(final - 1)
    for u in range(group):
        weigh(final, u)
    finish(final)

    def drain(copy, when):
        @pl.when(when)
        def _():
            copy.wait_send()

    for o in range(1, SPAN + 1):
        drain(seg_copy(o), me + o < n)
    for h in range(kv_heads):
        lane_here = (core == 0) | (h < TURNED)
        for j in range(REACH):
            slot = 2 * j + own_slot
            sends = lane_here & (chip >= j) & (chip < last)
            if j == REACH - 1:
                sends = sends & (core == 1)
            drain(hop(slot, h), sends)
            drain(side(slot, h), (lane_here & (chip >= j)) if j else core == 0)
        if h >= TURNED:
            drain(first_leg(h), (core == 1) & (chip < last))
            drain(second_leg(h), (core == 1) & (relayed < last))
            for j in range(1, REACH + 1):
                turned = (core == 0) & (chip >= j)
                if j >= 2:
                    drain(back_hop(2 * j, h), turned)
                if j < REACH:
                    drain(side(2 * j, h), turned)


def local(queries, keys, values, segment_ids):
    rows, width = queries.shape
    kv_width = keys.shape[1]
    heads, kv_heads = width // HD, kv_width // HD
    group = heads // kv_heads
    half = HD // 2
    freq = (ROPE_BASE ** (-(np.arange(half) * (2.0 / HD)))).astype(np.float32)
    freq = np.concatenate([freq, freq])[None]
    angle = (np.arange(rows, dtype=np.float32)[:, None] * freq).astype(np.float64)
    table = np.stack([np.cos(angle), np.sin(angle)]).astype(np.float32)
    in_hbm = pl.BlockSpec(memory_space=pltpu.HBM)
    bf16, f32 = jnp.bfloat16, jnp.float32
    slots = 2 * REACH + 1
    dma = pltpu.SemaphoreType.DMA
    return pl.pallas_call(
        functools.partial(kernel, kv_heads, group),
        out_shape=(
            pltpu.VMEM((rows, width), bf16),
            pltpu.VMEM((rows, kv_width), bf16),
        ),
        in_specs=[in_hbm] * 6,
        out_specs=(pl.BlockSpec(memory_space=pltpu.VMEM),) * 2,
        scratch_shapes=[
            pltpu.VMEM((SPAN + 1, 1, rows), jnp.int32),
            pltpu.VMEM((rows, width), bf16),
            pltpu.VMEM((slots, kv_heads, 2, rows, HD), bf16),
            pltpu.VMEM((2, rows, HD), f32),
            pltpu.VMEM((1, HD), f32),
            pltpu.VMEM((heads, HD, rows), bf16),
            pltpu.VMEM((rows, rows), f32),
            pltpu.VMEM((rows, HD), f32),
            pltpu.VMEM((rows, HD), f32),
            pltpu.VMEM((2, rows, HD), f32),
            pltpu.VMEM((2, rows, HD), f32),
            pltpu.VMEM((2 * rows, HD), bf16),
            pltpu.VMEM((HD + 16, 2 * rows), bf16),
            pltpu.VMEM((heads, 1, rows), f32),
            pltpu.VMEM((kv_heads, 8, HD), f32),
            pltpu.VMEM((heads, HD + 16, rows), f32),
            pltpu.VMEM((group, 2 * rows, rows), f32),
            pltpu.VMEM((group, 8, rows), f32),
            dma((4 + 2 * kv_heads,)),
            dma((SPAN,)),
            dma((SPAN,)),
            dma((slots, kv_heads)),
            dma((slots, kv_heads)),
            dma((slots, kv_heads)),
            pltpu.VMEM((kv_heads - TURNED, 2, rows, HD), bf16),
            dma((kv_heads - TURNED,)),
            dma((kv_heads - TURNED,)),
            dma((kv_heads - TURNED,)),
            dma((slots, kv_heads)),
        ],
        compiler_params=pltpu.CompilerParams(
            collective_id=0, has_side_effects=True, vmem_limit_bytes=64500000
        ),
    )(
        segment_ids.reshape(1, rows),
        queries,
        keys,
        values,
        jnp.asarray(table),
        jnp.asarray(freq),
    )


def solution(mesh):
    both = ("groups", "seq")
    return jax.shard_map(
        local,
        mesh=mesh,
        in_specs=(P(both, None), P(both, None), P(both, None), P(both)),
        out_specs=(P(both, None), P(both, None)),
        check_vma=False,
    )
```

```python
import functools
import math

import jax
import jax.numpy as jnp
import numpy as np
from jax import lax
from jax.experimental import pallas as pl
from jax.experimental.pallas import tpu as pltpu
from jax.sharding import PartitionSpec as P

HD = 128
SPAN = 7
REACH = 4
STRIP = 128
TURNED = 2
ROPE_BASE = 1000000.0
SCALE = float(HD ** (-0.5) * np.log2(np.e))
BIG = float(2.0**100)


def rotate(x, cosine, signed_sine):
    x = x.astype(jnp.float32)
    return x * cosine + pltpu.roll(x, HD // 2, 1) * signed_sine


def kernel(
    kv_heads,
    group,
    seg_in,
    q_in,
    k_in,
    v_in,
    table_in,
    freq_in,
    out,
    rk_out,
    segs,
    qraw,
    kv,
    tables,
    freq,
    qt,
    diag,
    own_cos,
    own_sin,
    blk_cos,
    blk_sin,
    kx,
    vt,
    top,
    anchor,
    acc,
    raw,
    peaks,
    in_sem,
    seg_send,
    seg_recv,
    hop_send,
    side_send,
    chain_send,
    via,
    via_send,
    via_recv,
    leg_send,
    kv_recv,
):
    rows = q_in.shape[0]
    half = HD // 2
    me = lax.axis_index("seq")
    n = lax.axis_size("seq")
    core = lax.rem(me, 2)
    own_slot = 1 - core
    chip = me // 2
    last = n // 2 - 1
    width = math.isqrt(n // 2)

    def device(offset):
        return {"seq": me + offset}

    def relay_of(source):
        return source // width * width + lax.rem(source + width - 2, width)

    def far_of(source):
        return jnp.minimum(source + REACH, last)

    relayed = chip // width * width + lax.rem(chip + 2, width)

    seg_load = pltpu.make_async_copy(seg_in, segs.at[0], in_sem.at[0])
    seg_load.start()
    kv_loads = []
    for h in range(kv_heads):
        cols = slice(h * HD, (h + 1) * HD)
        for w, src in ((0, k_in), (1, v_in)):
            load = pltpu.make_async_copy(
                src.at[:, cols], kv.at[own_slot, h, w], in_sem.at[4 + 2 * h + w]
            )
            load.start()
            kv_loads.append(load)
    freq_load = pltpu.make_async_copy(freq_in, freq, in_sem.at[1])
    freq_load.start()
    table_load = pltpu.make_async_copy(table_in, tables, in_sem.at[2])
    table_load.start()
    q_load = pltpu.make_async_copy(q_in, qraw, in_sem.at[3])
    q_load.start()

    barrier = pltpu.get_barrier_semaphore()

    def tell(rank, when):
        @pl.when(when)
        def _():
            pl.semaphore_signal(barrier, 1, device_id={"seq": rank})

    for o in range(1, SPAN + 1):
        tell(me - o, me >= o)
    tell(me + 1, (core == 0) & (chip >= 1))
    tell(me + 2, (core == 1) & (chip >= 1) & (chip < last))
    tell(2 * relayed + 1, (core == 1) & (relayed < last))
    tell(2 * relay_of(chip - REACH) + 1, (core == 1) & (chip >= REACH))
    for back in range(1, REACH):
        tell(2 * relay_of(chip - back) + 1, (core == 1) & (chip == last))
    receivers = jnp.minimum(SPAN, n - 1 - me) + jnp.where(
        core == 0,
        0,
        jnp.where(chip >= 1, 1, 0)
        + jnp.where(chip >= 2, 1, 0)
        + jnp.where(chip < last, 1, 0)
        + jnp.where(relayed < last, 1, 0),
    )
    pl.semaphore_wait(barrier, receivers)

    seg_load.wait()
    def seg_copy(o):
        return pltpu.make_async_remote_copy(
            src_ref=segs.at[0],
            dst_ref=segs.at[o],
            send_sem=seg_send.at[o - 1],
            recv_sem=seg_recv.at[o - 1],
            device_id=device(o),
        )

    for o in range(1, SPAN + 1):

        @pl.when(me + o < n)
        def _():
            seg_copy(o).start()

    def hop(slot, h):
        return pltpu.make_async_remote_copy(
            src_ref=kv.at[slot, h],
            dst_ref=kv.at[slot + 2, h],
            send_sem=hop_send.at[slot, h],
            recv_sem=kv_recv.at[slot + 2, h],
            device_id=device(2),
        )

    def last_hop(slot, h):
        return pltpu.make_async_remote_copy(
            src_ref=kv.at[slot, h],
            dst_ref=kv.at[slot + 2, h],
            send_sem=hop_send.at[slot, h],
            recv_sem=kv_recv.at[slot + 2, h],
            device_id=device(1),
        )

    def side(slot, h):
        return pltpu.make_async_remote_copy(
            src_ref=kv.at[slot, h],
            dst_ref=kv.at[slot, h],
            send_sem=side_send.at[slot, h],
            recv_sem=kv_recv.at[slot, h],
            device_id=device(1 - 2 * core),
        )

    def back_hop(slot, h):
        return pltpu.make_async_remote_copy(
            src_ref=kv.at[slot, h],
            dst_ref=kv.at[slot - 2, h],
            send_sem=chain_send.at[slot, h],
            recv_sem=kv_recv.at[slot - 2, h],
            device_id=device(-2),
        )

    def first_leg(h):
        return pltpu.make_async_remote_copy(
            src_ref=kv.at[own_slot, h],
            dst_ref=via.at[h - TURNED],
            send_sem=via_send.at[h - TURNED],
            recv_sem=via_recv.at[h - TURNED],
            device_id={"seq": 2 * relay_of(chip) + 1},
        )

    def second_leg(h):
        far = far_of(relayed)
        slot = 2 * (far - relayed)
        return pltpu.make_async_remote_copy(
            src_ref=via.at[h - TURNED],
            dst_ref=kv.at[slot, h],
            send_sem=leg_send.at[h - TURNED],
            recv_sem=kv_recv.at[slot, h],
            device_id={"seq": 2 * far + 1},
        )

    for h in range(kv_heads):
        kv_loads[2 * h].wait()
        kv_loads[2 * h + 1].wait()

        @pl.when((chip < last) & ((core == 0) | (h < TURNED)))
        def _():
            hop(own_slot, h).start()

        if h >= TURNED:

            @pl.when((chip < last) & (core == 1))
            def _():
                first_leg(h).start()

        @pl.when(core == 0)
        def _():
            side(own_slot, h).start()

    def blank(slot, carry):
        @pl.when(chip < slot // 2)
        def _():
            kv[slot] = jnp.zeros(kv.shape[1:], kv.dtype)

        return carry

    lax.fori_loop(2, 2 * REACH + 1, blank, 0)

    def relay(j, h, early):
        ahead = 2 * j + 1 - core
        before_ids = (chip < REACH) & (j < chip)
        mine = (j < REACH) & (chip >= j) & ((core == 0) | (h < TURNED))
        mine = mine & (before_ids if early else jnp.logical_not(before_ids))

        @pl.when(mine)
        def _():
            hop(ahead - 2, h).wait_recv()
            side(ahead, h).start()

        @pl.when(mine & (chip < last) & (j < REACH - 1))
        def _():
            hop(ahead, h).start()

        @pl.when(mine & (chip < last) & (j == REACH - 1) & (core == 1))
        def _():
            last_hop(ahead, h).start()

    def turn_back(early):
        when = (core == 1) & (relayed < last)
        when = when & ((chip < REACH) if early else (chip >= REACH))

        @pl.when(when)
        def _():
            for h in range(TURNED, kv_heads):
                first_leg(h).wait_recv()
                second_leg(h).start()

    freq_load.wait()
    table_load.wait()
    lane = lax.broadcasted_iota(jnp.int32, (rows, HD), 1)
    sublane = lax.broadcasted_iota(jnp.int32, (rows, HD), 0).astype(jnp.float32)
    sign = jnp.where(lane < half, -1.0, 1.0)
    freq_row = freq[...]
    seg_row = segs[0]
    seg_first = seg_row[:, :1]
    first_row = seg_row == seg_first
    seg_wide = jnp.broadcast_to(seg_row.astype(jnp.float32), (rows, rows))
    seg_tall = seg_wide.T
    key_at = lax.broadcasted_iota(jnp.int32, (rows, rows), 0)
    row_at = lax.broadcasted_iota(jnp.int32, (rows, rows), 1)
    same = seg_tall == seg_wide
    diag[...] = jnp.where(same & (key_at <= row_at), 0.0, -BIG)
    local_position = jnp.sum(
        jnp.where(same & (row_at < key_at), 1.0, 0.0), axis=1, keepdims=True
    )
    first_tall = seg_tall[:, :HD] == seg_first.astype(jnp.float32)
    local_angle = local_position * freq_row
    local_cos = jnp.cos(local_angle)
    local_sin = jnp.sin(local_angle)
    def clear(t, carry):
        top[t] = jnp.full((1, rows), -4.0 * BIG, jnp.float32)
        acc[t] = jnp.zeros(acc.shape[1:], jnp.float32)
        return carry

    lax.fori_loop(0, kv_heads * group, clear, 0)

    turn_back(True)

    def early_relay(i, carry):
        relay(i // kv_heads, lax.rem(i, kv_heads), True)
        return carry

    lax.fori_loop(kv_heads, (REACH - 1) * kv_heads, early_relay, 0)

    for o in range(1, SPAN + 1):

        @pl.when(me >= o)
        def _():
            seg_copy(o).wait_recv()

        @pl.when(me < o)
        def _():
            segs[o] = jnp.full((1, rows), -1, jnp.int32)

    hits = jnp.zeros_like(seg_row, jnp.float32)
    for o in range(1, SPAN + 1):
        hits += jnp.where(segs[o] == seg_first, 1.0, 0.0)
    before = jnp.sum(hits, axis=1, keepdims=True)
    base_angle = before * freq_row
    base_cos = jnp.where(first_tall, jnp.cos(base_angle), 1.0)
    base_sin = jnp.where(first_tall, jnp.sin(base_angle), 0.0)
    own_cos[...] = local_cos * base_cos - local_sin * base_sin
    own_sin[...] = (local_sin * base_cos + local_cos * base_sin) * sign

    for h in range(kv_heads):
        turned_keys = rotate(kv[own_slot, h, 0], own_cos[...], own_sin[...])
        anchor[h] = turned_keys[:8]
        rk_out[:, h * HD : (h + 1) * HD] = turned_keys.astype(jnp.bfloat16)

    q_load.wait()

    def turn(t, carry):
        at = pl.multiple_of(t * HD, HD)
        turned = rotate(qraw[:, pl.ds(at, HD)], own_cos[...], own_sin[...])
        qt[t] = turned.astype(jnp.bfloat16).T
        return carry

    lax.fori_loop(0, kv_heads * group, turn, 0)
    turn_back(False)

    chunks = (SPAN + 1) // 2 * kv_heads
    allowed_row = jnp.where(first_row, 0.0, -BIG)

    def split(q):
        part, i = q // kv_heads, lax.rem(q, kv_heads)
        pair = jnp.where(part < 2, i // TURNED, part)
        h = jnp.where(
            part < 2,
            lax.rem(i, TURNED) + TURNED * part,
            jnp.where(part == REACH - 1, lax.rem(i + TURNED, kv_heads), i),
        )
        return pair, h

    def slots_of(pair, h):
        forward = h < TURNED
        one = jnp.where(forward | (pair == 0), 2 * pair + 1 - core, 2 * pair + 1)
        two = jnp.where(
            forward,
            2 * pair + 2 - core,
            jnp.where((pair == 0) & (core == 1), 1, 2 * (REACH - pair)),
        )
        return one, two

    def missing(slot):
        return ((slot - 1 + core) * rows).astype(jnp.float32) - before

    def prepare(slots):
        for part, slot in enumerate(slots):
            own = slot == own_slot
            angle = -missing(slot) * freq_row
            c, s = jnp.cos(angle), jnp.sin(angle)

            @pl.when(own)
            def _():
                blk_cos[part] = own_cos[...]
                blk_sin[part] = own_sin[...]

            @pl.when(jnp.logical_not(own))
            def _():
                blk_cos[part] = tables[0] * c - tables[1] * s
                blk_sin[part] = (tables[1] * c + tables[0] * s) * sign

    def load_keys(q):
        pair, h = split(q)
        for part, slot in enumerate(slots_of(pair, h)):
            turned = rotate(kv[slot, h, 0], blk_cos[part], blk_sin[part])
            turned = jnp.where(sublane < missing(slot), anchor[h][:1], turned)
            kx[part * rows : (part + 1) * rows] = turned.astype(jnp.bfloat16)

    def load_values(q):
        pair, h = split(q)
        at = lax.broadcasted_iota(jnp.int32, (vt.shape[0] - HD, rows), 1).astype(jnp.float32)
        for part, slot in enumerate(slots_of(pair, h)):
            span = slice(part * rows, (part + 1) * rows)
            kept = jnp.where(sublane < missing(slot), 0.0, kv[slot, h, 1].astype(jnp.float32))
            vt[:HD, span] = kept.astype(jnp.bfloat16).T
            vt[HD:, span] = jnp.where(at < missing(slot), 0.0, 1.0).astype(jnp.bfloat16)

    def receive(q):
        pair, h = split(q)
        forward = h < TURNED
        back = h >= TURNED
        far = REACH - pair

        @pl.when(forward & (pair == 1))
        def _():
            @pl.when(h == 0)
            def _():
                for g in range(TURNED, kv_heads):
                    relay(1, g, False)

        turn_ahead = jnp.where(forward | (pair >= 2), pair + 1, 2)

        @pl.when(forward | (pair != 1))
        def _():
            relay(turn_ahead, h, False)

        chained = back & (core == 1) & (chip >= far)

        @pl.when(chained)
        def _():
            side(2 * far, h).wait_recv()

            @pl.when(far >= 2)
            def _():
                back_hop(2 * far, h).start()

            side(2 * far, h).start()

        one, two = slots_of(pair, h)

        @pl.when((h == 0) | (h == TURNED))
        def _():
            prepare((one, two))

        @pl.when(back & (pair > 0) & (core == 1) & (chip >= pair))
        def _():
            side(one, h).wait_recv()

        @pl.when((chip >= two // 2) & (forward | (core == 0) | (pair == 0)))
        def _():
            side(two, h).wait_recv()

    def score(q, u, own):
        _, h = split(q)
        t = h * group + u
        peak = None
        for at in range(0, 2 * rows, STRIP):
            scores = jnp.dot(kx[at : at + STRIP], qt[t], preferred_element_type=jnp.float32)
            if own:
                scores += diag[at : at + STRIP] if at < rows else allowed_row
            raw[u, at : at + STRIP] = scores
            top_here = jnp.max(scores.reshape(STRIP // 8, 8, rows), axis=0)
            peak = top_here if peak is None else jnp.maximum(peak, top_here)
        peaks[u] = peak if own else jnp.where(first_row, peak, -BIG)

    def weigh(q, u):
        pair, h = split(q)
        t = h * group + u
        old = top[t]
        peak = jnp.maximum(old, jnp.max(peaks[u], axis=0, keepdims=True))
        fade = jnp.exp2((old - peak) * SCALE)
        shift = jnp.where(first_row | (pair == 0), peak * SCALE, BIG)
        shift = jnp.broadcast_to(shift, (8, rows))
        top[t] = peak
        weights = []
        for at in range(0, 2 * rows, STRIP):
            scores = raw[u, at : at + STRIP].reshape(STRIP // 8, 8, rows)
            part = jnp.exp2(scores * SCALE - shift[None])
            weights.append(part.reshape(STRIP, rows).astype(jnp.bfloat16))
        acc[t] = acc[t] * fade + jnp.dot(
            vt[...], jnp.concatenate(weights, axis=0), preferred_element_type=jnp.float32
        )

    def finish(q):
        _, h = split(q)
        for g in range(group):
            t = h * group + g
            share = 1.0 / acc[t, HD : HD + 1]
            at = pl.multiple_of(t * HD, HD)
            out[:, pl.ds(at, HD)] = (acc[t, :HD] * share).astype(jnp.bfloat16).T

    def step(q, own):
        receive(q)
        load_keys(q)
        load_values(q - 1)
        for u in range(group):
            weigh(q - 1, u)
            score(q, u, own)

    first = jnp.int32(0)
    receive(first)
    load_keys(first)
    for u in range(group):
        score(first, u, True)

    def every_step(q, carry):
        @pl.when(q >= chunks - kv_heads + 2)
        def _():
            finish(q - 2)

        pair, _ = split(q)

        @pl.when(pair == 0)
        def _():
            step(q, True)

        @pl.when(pair > 0)
        def _():
            step(q, False)

        return carry

    lax.fori_loop(1, chunks, every_step, 0)
    final = jnp.int32(chunks - 1)
    load_values(final)
    finish(final - 1)
    for u in range(group):
        weigh(final, u)
    finish(final)

    def drain(copy, when):
        @pl.when(when)
        def _():
            copy.wait_send()

    for o in range(1, SPAN + 1):
        drain(seg_copy(o), me + o < n)
    for h in range(kv_heads):
        lane_here = (core == 0) | (h < TURNED)
        for j in range(REACH):
            slot = 2 * j + own_slot
            sends = lane_here & (chip >= j) & (chip < last)
            if j == REACH - 1:
                sends = sends & (core == 1)
            drain(hop(slot, h), sends)
            drain(side(slot, h), (lane_here & (chip >= j)) if j else core == 0)
        if h >= TURNED:
            drain(first_leg(h), (core == 1) & (chip < last))
            drain(second_leg(h), (core == 1) & (relayed < last))
            for j in range(1, REACH + 1):
                turned = (core == 1) & (chip >= j)
                if j >= 2:
                    drain(back_hop(2 * j, h), turned)
                drain(side(2 * j, h), turned)


def local(queries, keys, values, segment_ids):
    rows, width = queries.shape
    kv_width = keys.shape[1]
    heads, kv_heads = width // HD, kv_width // HD
    group = heads // kv_heads
    half = HD // 2
    freq = (ROPE_BASE ** (-(np.arange(half) * (2.0 / HD)))).astype(np.float32)
    freq = np.concatenate([freq, freq])[None]
    angle = (np.arange(rows, dtype=np.float32)[:, None] * freq).astype(np.float64)
    table = np.stack([np.cos(angle), np.sin(angle)]).astype(np.float32)
    in_hbm = pl.BlockSpec(memory_space=pltpu.HBM)
    bf16, f32 = jnp.bfloat16, jnp.float32
    slots = 2 * REACH + 1
    dma = pltpu.SemaphoreType.DMA
    return pl.pallas_call(
        functools.partial(kernel, kv_heads, group),
        out_shape=(
            pltpu.VMEM((rows, width), bf16),
            pltpu.VMEM((rows, kv_width), bf16),
        ),
        in_specs=[in_hbm] * 6,
        out_specs=(pl.BlockSpec(memory_space=pltpu.VMEM),) * 2,
        scratch_shapes=[
            pltpu.VMEM((SPAN + 1, 1, rows), jnp.int32),
            pltpu.VMEM((rows, width), bf16),
            pltpu.VMEM((slots, kv_heads, 2, rows, HD), bf16),
            pltpu.VMEM((2, rows, HD), f32),
            pltpu.VMEM((1, HD), f32),
            pltpu.VMEM((heads, HD, rows), bf16),
            pltpu.VMEM((rows, rows), f32),
            pltpu.VMEM((rows, HD), f32),
            pltpu.VMEM((rows, HD), f32),
            pltpu.VMEM((2, rows, HD), f32),
            pltpu.VMEM((2, rows, HD), f32),
            pltpu.VMEM((2 * rows, HD), bf16),
            pltpu.VMEM((HD + 16, 2 * rows), bf16),
            pltpu.VMEM((heads, 1, rows), f32),
            pltpu.VMEM((kv_heads, 8, HD), f32),
            pltpu.VMEM((heads, HD + 16, rows), f32),
            pltpu.VMEM((group, 2 * rows, rows), f32),
            pltpu.VMEM((group, 8, rows), f32),
            dma((4 + 2 * kv_heads,)),
            dma((SPAN,)),
            dma((SPAN,)),
            dma((slots, kv_heads)),
            dma((slots, kv_heads)),
            dma((slots, kv_heads)),
            pltpu.VMEM((kv_heads - TURNED, 2, rows, HD), bf16),
            dma((kv_heads - TURNED,)),
            dma((kv_heads - TURNED,)),
            dma((kv_heads - TURNED,)),
            dma((slots, kv_heads)),
        ],
        compiler_params=pltpu.CompilerParams(
            collective_id=0, has_side_effects=True, vmem_limit_bytes=64500000
        ),
    )(
        segment_ids.reshape(1, rows),
        queries,
        keys,
        values,
        jnp.asarray(table),
        jnp.asarray(freq),
    )


def solution(mesh):
    both = ("groups", "seq")
    return jax.shard_map(
        local,
        mesh=mesh,
        in_specs=(P(both, None), P(both, None), P(both, None), P(both)),
        out_specs=(P(both, None), P(both, None)),
        check_vma=False,
    )
```

```python
import functools
import math

import jax
import jax.numpy as jnp
import numpy as np
from jax import lax
from jax.experimental import pallas as pl
from jax.experimental.pallas import tpu as pltpu
from jax.sharding import PartitionSpec as P

HD = 128
SPAN = 7
REACH = 4
STRIP = 128
TURNED = 2
ROPE_BASE = 1000000.0
SCALE = float(HD ** (-0.5) * np.log2(np.e))
BIG = float(2.0**100)


def rotate(x, cosine, signed_sine):
    x = x.astype(jnp.float32)
    return x * cosine + pltpu.roll(x, HD // 2, 1) * signed_sine


def kernel(
    kv_heads,
    group,
    seg_in,
    q_in,
    k_in,
    v_in,
    table_in,
    freq_in,
    out,
    rk_out,
    segs,
    qraw,
    kv,
    tables,
    freq,
    qt,
    diag,
    own_cos,
    own_sin,
    blk_cos,
    blk_sin,
    kx,
    vt,
    top,
    anchor,
    acc,
    raw,
    peaks,
    in_sem,
    seg_send,
    seg_recv,
    hop_send,
    side_send,
    chain_send,
    via,
    via_send,
    via_recv,
    leg_send,
    kv_recv,
):
    rows = q_in.shape[0]
    half = HD // 2
    me = lax.axis_index("seq")
    n = lax.axis_size("seq")
    core = lax.rem(me, 2)
    own_slot = 1 - core
    chip = me // 2
    last = n // 2 - 1
    width = math.isqrt(n // 2)

    def device(offset):
        return {"seq": me + offset}

    def relay_of(source):
        return source // width * width + lax.rem(source + width - 2, width)

    def far_of(source):
        return jnp.minimum(source + REACH, last)

    relayed = chip // width * width + lax.rem(chip + 2, width)

    seg_load = pltpu.make_async_copy(seg_in, segs.at[0], in_sem.at[0])
    seg_load.start()
    kv_loads = []
    for h in range(kv_heads):
        cols = slice(h * HD, (h + 1) * HD)
        for w, src in ((0, k_in), (1, v_in)):
            load = pltpu.make_async_copy(
                src.at[:, cols], kv.at[own_slot, h, w], in_sem.at[4 + 2 * h + w]
            )
            load.start()
            kv_loads.append(load)
    freq_load = pltpu.make_async_copy(freq_in, freq, in_sem.at[1])
    freq_load.start()
    table_load = pltpu.make_async_copy(table_in, tables, in_sem.at[2])
    table_load.start()
    q_load = pltpu.make_async_copy(q_in, qraw, in_sem.at[3])
    q_load.start()

    barrier = pltpu.get_barrier_semaphore()

    def tell(rank, when):
        @pl.when(when)
        def _():
            pl.semaphore_signal(barrier, 1, device_id={"seq": rank})

    for o in range(1, SPAN + 1):
        tell(me - o, me >= o)
    tell(me + 1, (core == 0) & (chip >= 1))
    tell(me + 2, (core == 1) & (chip >= 1) & (chip < last))
    tell(2 * relayed + 1, (core == 1) & (relayed < last))
    tell(2 * relay_of(chip - REACH) + 1, (core == 1) & (chip >= REACH))
    for back in range(1, REACH):
        tell(2 * relay_of(chip - back) + 1, (core == 1) & (chip == last))
    receivers = jnp.minimum(SPAN, n - 1 - me) + jnp.where(
        core == 0,
        0,
        jnp.where(chip >= 1, 1, 0)
        + jnp.where(chip >= 2, 1, 0)
        + jnp.where(chip < last, 1, 0)
        + jnp.where(relayed < last, 1, 0),
    )
    pl.semaphore_wait(barrier, receivers)

    seg_load.wait()
    def seg_copy(o):
        return pltpu.make_async_remote_copy(
            src_ref=segs.at[0],
            dst_ref=segs.at[o],
            send_sem=seg_send.at[o - 1],
            recv_sem=seg_recv.at[o - 1],
            device_id=device(o),
        )

    for o in range(1, SPAN + 1):

        @pl.when(me + o < n)
        def _():
            seg_copy(o).start()

    def hop(slot, h):
        return pltpu.make_async_remote_copy(
            src_ref=kv.at[slot, h],
            dst_ref=kv.at[slot + 2, h],
            send_sem=hop_send.at[slot, h],
            recv_sem=kv_recv.at[slot + 2, h],
            device_id=device(2),
        )

    def last_hop(slot, h):
        return pltpu.make_async_remote_copy(
            src_ref=kv.at[slot, h],
            dst_ref=kv.at[slot + 2, h],
            send_sem=hop_send.at[slot, h],
            recv_sem=kv_recv.at[slot + 2, h],
            device_id=device(1),
        )

    def side(slot, h):
        return pltpu.make_async_remote_copy(
            src_ref=kv.at[slot, h],
            dst_ref=kv.at[slot, h],
            send_sem=side_send.at[slot, h],
            recv_sem=kv_recv.at[slot, h],
            device_id=device(1 - 2 * core),
        )

    def back_hop(slot, h):
        return pltpu.make_async_remote_copy(
            src_ref=kv.at[slot, h],
            dst_ref=kv.at[slot - 2, h],
            send_sem=chain_send.at[slot, h],
            recv_sem=kv_recv.at[slot - 2, h],
            device_id=device(-2),
        )

    def first_leg(h):
        return pltpu.make_async_remote_copy(
            src_ref=kv.at[own_slot, h],
            dst_ref=via.at[h - TURNED],
            send_sem=via_send.at[h - TURNED],
            recv_sem=via_recv.at[h - TURNED],
            device_id={"seq": 2 * relay_of(chip) + 1},
        )

    def second_leg(h):
        far = far_of(relayed)
        slot = 2 * (far - relayed)
        return pltpu.make_async_remote_copy(
            src_ref=via.at[h - TURNED],
            dst_ref=kv.at[slot, h],
            send_sem=leg_send.at[h - TURNED],
            recv_sem=kv_recv.at[slot, h],
            device_id={"seq": 2 * far + 1},
        )

    for h in range(kv_heads):
        kv_loads[2 * h].wait()
        kv_loads[2 * h + 1].wait()

        @pl.when((chip < last) & ((core == 0) | (h < TURNED)))
        def _():
            hop(own_slot, h).start()

        if h >= TURNED:

            @pl.when((chip < last) & (core == 1))
            def _():
                first_leg(h).start()

        @pl.when(core == 0)
        def _():
            side(own_slot, h).start()

    def blank(slot, carry):
        @pl.when(chip < slot // 2)
        def _():
            kv[slot] = jnp.zeros(kv.shape[1:], kv.dtype)

        return carry

    lax.fori_loop(2, 2 * REACH + 1, blank, 0)

    def relay(j, h, early):
        ahead = 2 * j + 1 - core
        before_ids = (chip < REACH) & (j < chip)
        mine = (j < REACH) & (chip >= j) & ((core == 0) | (h < TURNED))
        mine = mine & (before_ids if early else jnp.logical_not(before_ids))

        @pl.when(mine)
        def _():
            hop(ahead - 2, h).wait_recv()
            side(ahead, h).start()

        @pl.when(mine & (chip < last) & (j < REACH - 1))
        def _():
            hop(ahead, h).start()

        @pl.when(mine & (chip < last) & (j == REACH - 1) & (core == 1))
        def _():
            last_hop(ahead, h).start()

    def turn_back(early):
        when = (core == 1) & (relayed < last)
        when = when & ((chip < REACH) if early else (chip >= REACH))

        @pl.when(when)
        def _():
            for h in range(TURNED, kv_heads):
                first_leg(h).wait_recv()
                second_leg(h).start()

    freq_load.wait()
    table_load.wait()
    lane = lax.broadcasted_iota(jnp.int32, (rows, HD), 1)
    sublane = lax.broadcasted_iota(jnp.int32, (rows, HD), 0).astype(jnp.float32)
    sign = jnp.where(lane < half, -1.0, 1.0)
    freq_row = freq[...]
    seg_row = segs[0]
    seg_first = seg_row[:, :1]
    first_row = seg_row == seg_first
    seg_wide = jnp.broadcast_to(seg_row.astype(jnp.float32), (rows, rows))
    seg_tall = seg_wide.T
    key_at = lax.broadcasted_iota(jnp.int32, (rows, rows), 0)
    row_at = lax.broadcasted_iota(jnp.int32, (rows, rows), 1)
    same = seg_tall == seg_wide
    diag[...] = jnp.where(same & (key_at <= row_at), 0.0, -BIG)
    local_position = jnp.sum(
        jnp.where(same & (row_at < key_at), 1.0, 0.0), axis=1, keepdims=True
    )
    first_tall = seg_tall[:, :HD] == seg_first.astype(jnp.float32)
    local_angle = local_position * freq_row
    local_cos = jnp.cos(local_angle)
    local_sin = jnp.sin(local_angle)
    def clear(t, carry):
        top[t] = jnp.full((1, rows), -4.0 * BIG, jnp.float32)
        acc[t] = jnp.zeros(acc.shape[1:], jnp.float32)
        return carry

    lax.fori_loop(0, kv_heads * group, clear, 0)

    turn_back(True)

    def early_relay(i, carry):
        relay(i // kv_heads, lax.rem(i, kv_heads), True)
        return carry

    lax.fori_loop(kv_heads, (REACH - 1) * kv_heads, early_relay, 0)

    for o in range(1, SPAN + 1):

        @pl.when(me >= o)
        def _():
            seg_copy(o).wait_recv()

        @pl.when(me < o)
        def _():
            segs[o] = jnp.full((1, rows), -1, jnp.int32)

    hits = jnp.zeros_like(seg_row, jnp.float32)
    for o in range(1, SPAN + 1):
        hits += jnp.where(segs[o] == seg_first, 1.0, 0.0)
    before = jnp.sum(hits, axis=1, keepdims=True)
    base_angle = before * freq_row
    base_cos = jnp.where(first_tall, jnp.cos(base_angle), 1.0)
    base_sin = jnp.where(first_tall, jnp.sin(base_angle), 0.0)
    own_cos[...] = local_cos * base_cos - local_sin * base_sin
    own_sin[...] = (local_sin * base_cos + local_cos * base_sin) * sign

    for h in range(kv_heads):
        turned_keys = rotate(kv[own_slot, h, 0], own_cos[...], own_sin[...])
        anchor[h] = turned_keys[:8]
        rk_out[:, h * HD : (h + 1) * HD] = turned_keys.astype(jnp.bfloat16)

    q_load.wait()

    def turn(t, carry):
        at = pl.multiple_of(t * HD, HD)
        turned = rotate(qraw[:, pl.ds(at, HD)], own_cos[...], own_sin[...])
        qt[t] = turned.astype(jnp.bfloat16).T
        return carry

    lax.fori_loop(0, kv_heads * group, turn, 0, unroll=4)
    turn_back(False)

    chunks = (SPAN + 1) // 2 * kv_heads
    allowed_row = jnp.where(first_row, 0.0, -BIG)

    def split(q):
        part, i = q // kv_heads, lax.rem(q, kv_heads)
        pair = jnp.where(part < 2, i // TURNED, part)
        h = jnp.where(
            part < 2,
            lax.rem(i, TURNED) + TURNED * part,
            jnp.where(part == REACH - 1, lax.rem(i + TURNED, kv_heads), i),
        )
        return pair, h

    def slots_of(pair, h):
        forward = h < TURNED
        one = jnp.where(forward | (pair == 0), 2 * pair + 1 - core, 2 * pair + 1)
        two = jnp.where(
            forward,
            2 * pair + 2 - core,
            jnp.where((pair == 0) & (core == 1), 1, 2 * (REACH - pair)),
        )
        return one, two

    def missing(slot):
        return ((slot - 1 + core) * rows).astype(jnp.float32) - before

    def prepare(slots):
        for part, slot in enumerate(slots):
            own = slot == own_slot
            angle = -missing(slot) * freq_row
            c, s = jnp.cos(angle), jnp.sin(angle)

            @pl.when(own)
            def _():
                blk_cos[part] = own_cos[...]
                blk_sin[part] = own_sin[...]

            @pl.when(jnp.logical_not(own))
            def _():
                blk_cos[part] = tables[0] * c - tables[1] * s
                blk_sin[part] = (tables[1] * c + tables[0] * s) * sign

    def load_keys(q):
        pair, h = split(q)
        for part, slot in enumerate(slots_of(pair, h)):
            turned = rotate(kv[slot, h, 0], blk_cos[part], blk_sin[part])
            turned = jnp.where(sublane < missing(slot), anchor[h][:1], turned)
            kx[part * rows : (part + 1) * rows] = turned.astype(jnp.bfloat16)

    def load_values(q):
        pair, h = split(q)
        at = lax.broadcasted_iota(jnp.int32, (vt.shape[0] - HD, rows), 1).astype(jnp.float32)
        for part, slot in enumerate(slots_of(pair, h)):
            span = slice(part * rows, (part + 1) * rows)
            kept = jnp.where(sublane < missing(slot), 0.0, kv[slot, h, 1].astype(jnp.float32))
            vt[:HD, span] = kept.astype(jnp.bfloat16).T
            vt[HD:, span] = jnp.where(at < missing(slot), 0.0, 1.0).astype(jnp.bfloat16)

    def receive(q):
        pair, h = split(q)
        forward = h < TURNED
        back = h >= TURNED
        far = REACH - pair

        @pl.when(forward & (pair == 1))
        def _():
            @pl.when(h == 0)
            def _():
                for g in range(TURNED, kv_heads):
                    relay(1, g, False)

        turn_ahead = jnp.where(forward | (pair >= 2), pair + 1, 2)

        @pl.when(forward | (pair != 1))
        def _():
            relay(turn_ahead, h, False)

        chained = back & (core == 1) & (chip >= far)

        @pl.when(chained)
        def _():
            side(2 * far, h).wait_recv()

            @pl.when(far >= 2)
            def _():
                back_hop(2 * far, h).start()

            side(2 * far, h).start()

        one, two = slots_of(pair, h)

        @pl.when((h == 0) | (h == TURNED))
        def _():
            prepare((one, two))

        @pl.when(back & (pair > 0) & (core == 1) & (chip >= pair))
        def _():
            side(one, h).wait_recv()

        @pl.when((chip >= two // 2) & (forward | (core == 0) | (pair == 0)))
        def _():
            side(two, h).wait_recv()

    def score(q, u, own):
        _, h = split(q)
        t = h * group + u
        peak = None
        for at in range(0, 2 * rows, STRIP):
            scores = jnp.dot(kx[at : at + STRIP], qt[t], preferred_element_type=jnp.float32)
            if own:
                scores += diag[at : at + STRIP] if at < rows else allowed_row
            raw[u, at : at + STRIP] = scores
            top_here = jnp.max(scores.reshape(STRIP // 8, 8, rows), axis=0)
            peak = top_here if peak is None else jnp.maximum(peak, top_here)
        peaks[u] = peak if own else jnp.where(first_row, peak, -BIG)

    def weigh(q, u):
        pair, h = split(q)
        t = h * group + u
        old = top[t]
        peak = jnp.maximum(old, jnp.max(peaks[u], axis=0, keepdims=True))
        fade = jnp.exp2((old - peak) * SCALE)
        shift = jnp.where(first_row | (pair == 0), peak * SCALE, BIG)
        shift = jnp.broadcast_to(shift, (8, rows))
        top[t] = peak
        weights = []
        for at in range(0, 2 * rows, STRIP):
            scores = raw[u, at : at + STRIP].reshape(STRIP // 8, 8, rows)
            part = jnp.exp2(scores * SCALE - shift[None])
            weights.append(part.reshape(STRIP, rows).astype(jnp.bfloat16))
        acc[t] = acc[t] * fade + jnp.dot(
            vt[...], jnp.concatenate(weights, axis=0), preferred_element_type=jnp.float32
        )

    def finish(q):
        _, h = split(q)
        for g in range(group):
            t = h * group + g
            share = 1.0 / acc[t, HD : HD + 1]
            at = pl.multiple_of(t * HD, HD)
            out[:, pl.ds(at, HD)] = (acc[t, :HD] * share).astype(jnp.bfloat16).T

    short = chip < REACH - 1

    def taken(q):
        one, two = slots_of(*split(q))
        return (chip >= one // 2) | (chip >= two // 2)

    def step(q, held, own):
        load_keys(q)
        load_values(held)
        for u in range(group):
            weigh(held, u)
            score(q, u, own)

    first = jnp.int32(0)
    receive(first)
    load_keys(first)
    for u in range(group):
        score(first, u, True)

    def every_step(q, held):
        @pl.when((q >= chunks - kv_heads + 2) & jnp.logical_not(short))
        def _():
            finish(q - 2)

        receive(q)
        pair, _ = split(q)

        @pl.when(pair == 0)
        def _():
            step(q, held, True)

        @pl.when((pair > 0) & taken(q))
        def _():
            step(q, held, False)

        return jnp.where(taken(q), q, held)

    held = lax.fori_loop(1, chunks, every_step, first)
    final = jnp.int32(chunks - 1)
    load_values(held)
    finish(final - 1)
    for u in range(group):
        weigh(held, u)

    def finish_late(i, carry):
        finish(final - i)
        return carry

    lax.fori_loop(2, jnp.where(short, kv_heads, 2), finish_late, 0)
    finish(final)

    def drain(copy, when):
        @pl.when(when)
        def _():
            copy.wait_send()

    for o in range(1, SPAN + 1):
        drain(seg_copy(o), me + o < n)
    for h in range(kv_heads):
        lane_here = (core == 0) | (h < TURNED)
        for j in range(REACH):
            slot = 2 * j + own_slot
            sends = lane_here & (chip >= j) & (chip < last)
            if j == REACH - 1:
                sends = sends & (core == 1)
            drain(hop(slot, h), sends)
            drain(side(slot, h), (lane_here & (chip >= j)) if j else core == 0)
        if h >= TURNED:
            drain(first_leg(h), (core == 1) & (chip < last))
            drain(second_leg(h), (core == 1) & (relayed < last))
            for j in range(1, REACH + 1):
                turned = (core == 1) & (chip >= j)
                if j >= 2:
                    drain(back_hop(2 * j, h), turned)
                drain(side(2 * j, h), turned)


def local(queries, keys, values, segment_ids):
    rows, width = queries.shape
    kv_width = keys.shape[1]
    heads, kv_heads = width // HD, kv_width // HD
    group = heads // kv_heads
    half = HD // 2
    freq = (ROPE_BASE ** (-(np.arange(half) * (2.0 / HD)))).astype(np.float32)
    freq = np.concatenate([freq, freq])[None]
    angle = (np.arange(rows, dtype=np.float32)[:, None] * freq).astype(np.float64)
    table = np.stack([np.cos(angle), np.sin(angle)]).astype(np.float32)
    in_hbm = pl.BlockSpec(memory_space=pltpu.HBM)
    bf16, f32 = jnp.bfloat16, jnp.float32
    slots = 2 * REACH + 1
    dma = pltpu.SemaphoreType.DMA
    return pl.pallas_call(
        functools.partial(kernel, kv_heads, group),
        out_shape=(
            pltpu.VMEM((rows, width), bf16),
            pltpu.VMEM((rows, kv_width), bf16),
        ),
        in_specs=[in_hbm] * 6,
        out_specs=(pl.BlockSpec(memory_space=pltpu.VMEM),) * 2,
        scratch_shapes=[
            pltpu.VMEM((SPAN + 1, 1, rows), jnp.int32),
            pltpu.VMEM((rows, width), bf16),
            pltpu.VMEM((slots, kv_heads, 2, rows, HD), bf16),
            pltpu.VMEM((2, rows, HD), f32),
            pltpu.VMEM((1, HD), f32),
            pltpu.VMEM((heads, HD, rows), bf16),
            pltpu.VMEM((rows, rows), f32),
            pltpu.VMEM((rows, HD), f32),
            pltpu.VMEM((rows, HD), f32),
            pltpu.VMEM((2, rows, HD), f32),
            pltpu.VMEM((2, rows, HD), f32),
            pltpu.VMEM((2 * rows, HD), bf16),
            pltpu.VMEM((HD + 16, 2 * rows), bf16),
            pltpu.VMEM((heads, 1, rows), f32),
            pltpu.VMEM((kv_heads, 8, HD), f32),
            pltpu.VMEM((heads, HD + 16, rows), f32),
            pltpu.VMEM((group, 2 * rows, rows), f32),
            pltpu.VMEM((group, 8, rows), f32),
            dma((4 + 2 * kv_heads,)),
            dma((SPAN,)),
            dma((SPAN,)),
            dma((slots, kv_heads)),
            dma((slots, kv_heads)),
            dma((slots, kv_heads)),
            pltpu.VMEM((kv_heads - TURNED, 2, rows, HD), bf16),
            dma((kv_heads - TURNED,)),
            dma((kv_heads - TURNED,)),
            dma((kv_heads - TURNED,)),
            dma((slots, kv_heads)),
        ],
        compiler_params=pltpu.CompilerParams(
            collective_id=0, has_side_effects=True, vmem_limit_bytes=64500000
        ),
    )(
        segment_ids.reshape(1, rows),
        queries,
        keys,
        values,
        jnp.asarray(table),
        jnp.asarray(freq),
    )


def solution(mesh):
    both = ("groups", "seq")
    return jax.shard_map(
        local,
        mesh=mesh,
        in_specs=(P(both, None), P(both, None), P(both, None), P(both)),
        out_specs=(P(both, None), P(both, None)),
        check_vma=False,
    )
```
